128 devices in a mesh: sub: 64 (over x_hi, z, y, core), tm: 2 (over x_lo).
Axes of the slice: x: 4 (x_hi: 2, x_lo: 2; x = x_hi * 2 + x_lo), y: 4, z: 4, core: 2. Of those that a mesh axis runs over, the one named last changes fastest.
Arguments:
- voltages: bfloat16 [768, 2, 96, 2048], P('sub', None, None, 'tm'), may hold values from -6 to 6
- pointing_table: bfloat16 [768, 2, 320, 96], P('sub'), may hold values from -0.4375 to 0.4375
- beam_pointing: int32 [256], replicated, may hold values from 0 to 319
- subband_order: int32 [768], replicated, may hold values from 0 to 767, each once
- live_subbands: int32 [1], replicated, may hold values from 728 to 768
- filter_taps: float32 [16, 16], replicated, may hold values from -0.36 to 0.36
Outputs:
- synthesised: bfloat16 [256, 48, 2, 32768], P('sub', None, None, 'tm')
The draws below stay inside these ranges and needn't reach their ends.
Inputs may be any that keep to these rules, and one draw needn't show every extreme that they name: `subband_order`: each slot is named by exactly one frequency.
All inputs are finite; a program needn't handle non-finite values.
Results may differ from the reference program's by a relative error of at most 0.0052.
Values may be sent and summed in bfloat16 or wider, within the bound.
A program may use at most 192 MiB of HBM per device.

```python
import math
import jax
import jax.numpy as jnp
from jax import lax

INPUTS = 96
BEAMS = 256
POINTINGS = 320
CHAN = 16
TAPS = 16
SUBBANDS = 768
TIME = 2048


def draw_live_subbands(key, part):
    span = 2 * CHAN + CHAN // 2
    raw = jax.random.randint(jax.random.fold_in(key, 7919), (1,), -span, span + 1, dtype=jnp.int32)
    missing = jnp.maximum(raw, 0)
    return (SUBBANDS - missing).astype(jnp.int32)


def place_ends(drawn, rng, smallest, top_value):
    longest = drawn.shape.index(max(drawn.shape))
    spots = []
    for shift in (0, 1):
        where = [jax.random.randint(jax.random.fold_in(rng, axis), (), 0, length) for axis, length in enumerate(drawn.shape)]
        where[longest] = (where[longest] + shift) % drawn.shape[longest]
        spots.append(tuple(where))
    return drawn.at[spots[0]].set(smallest).at[spots[1]].set(top_value)


def levels(key, shape, cuts, least, top_value):
    def one(axis_at, blocks):
        steps = jax.random.uniform(jax.random.fold_in(jax.random.fold_in(key, 6), axis_at), (blocks,), jnp.float32, least / len(cuts), top_value / len(cuts))
        return jnp.repeat(jnp.exp(steps), shape[axis_at] // blocks).reshape((-1,) + (1,) * (len(shape) - axis_at - 1))

    loudness = one(*cuts[0])
    for cut in cuts[1:]:
        loudness = loudness * one(*cut)
    return loudness


def gaussian(own_key, dims, spread, bound, pieces=(), held_as=jnp.bfloat16):
    array = spread * jax.random.normal(own_key, dims, jnp.float32)
    if pieces:
        array = array * levels(own_key, dims, pieces, -0.22, 0.18)
    return jnp.clip(array, -bound, bound).astype(held_as)


def setup_inputs(seed: int = 0) -> dict:
    key_of = jax.random.split(jax.random.key(seed), 7)
    return {
        "voltages": gaussian(key_of[0], (SUBBANDS, 2, INPUTS, TIME), 1.0, 6.0, ((0, 64), (3, 2))),
        "pointing_table": gaussian(key_of[1], (SUBBANDS, 2, POINTINGS, INPUTS), (2 * INPUTS) ** -0.5, 0.4375, ((0, 64),)),
        "beam_pointing": place_ends(jax.random.randint(key_of[2], (BEAMS,), 0, POINTINGS), jax.random.fold_in(key_of[2], 1), 0, POINTINGS - 1).astype(jnp.int32),
        "subband_order": jax.random.permutation(key_of[3], SUBBANDS).astype(jnp.int32),
        "live_subbands": draw_live_subbands(jax.random.fold_in(key_of[6], 71), 0),
        "filter_taps": gaussian(key_of[5], (TAPS, CHAN), 0.06, 0.36, (), jnp.float32),
    }


def inverse_table(channel_count):
    channel_index = jnp.arange(channel_count, dtype=jnp.int32)
    phase = (jnp.outer(channel_index, channel_index) % channel_count).astype(jnp.float32) * (2.0 * math.pi / channel_count)
    cosine = jnp.cos(phase).astype(jnp.bfloat16)
    sine_table = jnp.sin(phase).astype(jnp.bfloat16)
    upper_rows = jnp.stack([cosine, -sine_table], axis=1)
    lower_rows = jnp.stack([sine_table, cosine], axis=1)
    return jnp.stack([upper_rows, lower_rows], axis=0)


def reference(voltages, pointing_table, beam_pointing, subband_order, live_subbands, filter_taps):
    highest = lax.Precision.HIGHEST

    def form_subband(subband_pair):
        table_rows, signal = subband_pair
        chosen = jnp.take(table_rows, beam_pointing, axis=1).astype(jnp.float32)
        signal = signal.astype(jnp.float32)
        real_part = jnp.dot(chosen[0], signal[0], precision=highest) - jnp.dot(chosen[1], signal[1], precision=highest)
        imag_part = jnp.dot(chosen[1], signal[0], precision=highest) + jnp.dot(chosen[0], signal[1], precision=highest)
        return jnp.stack([real_part, imag_part], axis=1).astype(jnp.bfloat16)

    formed = lax.map(form_subband, (pointing_table, voltages))
    inverse_rows = inverse_table(CHAN).astype(jnp.float32)
    live_mask = jnp.arange(SUBBANDS, dtype=jnp.int32) < live_subbands[0]
    length = formed.shape[3]

    def synth_beam(beam_index):
        beam_rows = lax.dynamic_index_in_dim(formed, beam_index, 1, keepdims=False)
        spectrum = jnp.take(beam_rows, subband_order, axis=0)
        spectrum = jnp.where(live_mask[:, None, None], spectrum, jnp.zeros_like(spectrum))
        grouped = spectrum.astype(jnp.float32).reshape(SUBBANDS // CHAN, CHAN, 2, length)
        channels = jnp.einsum('qkpc,gcpt->gqkt', inverse_rows, grouped, precision=highest)
        extended = jnp.pad(channels, ((0, 0), (0, 0), (0, 0), (TAPS - 1, 0)))
        running = jnp.zeros_like(channels)
        for tap_index in range(TAPS):
            offset = TAPS - 1 - tap_index
            running = running + filter_taps[tap_index][:, None] * extended[..., offset:offset + length]
        return jnp.swapaxes(running, 2, 3).reshape(SUBBANDS // CHAN, 2, length * CHAN).astype(jnp.bfloat16)

    return lax.map(synth_beam, jnp.arange(BEAMS, dtype=jnp.int32))
```

```python
import functools

import jax
import jax.numpy as jnp
import numpy as np
from jax import lax
from jax.experimental import pallas as pl
from jax.experimental.pallas import tpu as pltpu
from jax.sharding import PartitionSpec as P

MESH = pl.DeviceIdType.MESH
BF = jnp.bfloat16
F32 = jnp.float32
NT = (((1,), (1,)), ((), ()))
EARLY = 3


def coefficient_rows():
    k = np.arange(16)
    phase = ((np.outer(k, k) % 16).astype(np.float32) * np.float32(2.0 * np.pi / 16)).astype(np.float32)
    cos = np.cos(phase).astype(jnp.bfloat16).astype(np.float32)
    sin = np.sin(phase).astype(jnp.bfloat16).astype(np.float32)
    rows = np.stack([np.stack([cos, -sin]), np.stack([sin, cos])])
    rows = rows.transpose(0, 1, 3, 2).reshape(64, 16)
    return np.tile(rows, (1, 8)).astype(np.float32)


def iota(shape, dim):
    return lax.broadcasted_iota(jnp.int32, shape, dim)


def build_filter(taps_ref, coef_ref, filt_ref):
    repeat = (iota((16, 128), 1) % 16 == iota((16, 128), 0)).astype(F32)
    taps = jnp.dot(taps_ref[...], repeat, precision=lax.Precision.HIGHEST, preferred_element_type=F32)
    lag = iota((8, 128), 1) // 16 - iota((8, 128), 0)
    for d in range(3):
        tap = jnp.zeros((8, 128), F32)
        for j in range(16):
            tap = jnp.where(lag + 8 * d == j, jnp.broadcast_to(taps[j : j + 1], (8, 128)), tap)
        for q in range(2):
            for c in range(16):
                block = [
                    tap * coef_ref[(2 * q + p) * 16 + c : (2 * q + p) * 16 + c + 1, :] for p in range(2)
                ]
                filt_ref[d, 16 * c : 16 * c + 16, 128 * q : 128 * q + 128] = jnp.concatenate(
                    block, axis=0
                ).astype(BF)


def band(rows_ref, order_ref, live, group):
    parts = []
    for c in range(16):
        f = group * 16 + c
        part = rows_ref[order_ref[f]]
        parts.append(jnp.where(f < live, part, jnp.zeros_like(part)))
    return jnp.concatenate(parts, axis=0)


def synthesise(bands, groups, carry_ref, filt_ref, one_ref, two_ref, mix_ref):
    n = len(bands)
    zt = jnp.concatenate([z.T for z in bands], axis=0)
    now = jnp.dot(zt, filt_ref[0], preferred_element_type=F32)
    one = jnp.dot(zt, filt_ref[1], preferred_element_type=F32)
    two = jnp.dot(zt, filt_ref[2], preferred_element_type=F32)
    outs = []
    for i in range(n):
        one_ref[i, 8:136, :] = one[128 * i : 128 * i + 128]
        two_ref[i, 8:136, :] = two[128 * i : 128 * i + 128]
        one_ref[i, 7:8, :] = carry_ref[0, pl.ds(groups[i], 1), :]
        two_ref[i, 7:8, :] = carry_ref[1, pl.ds(groups[i], 1), :]
        two_ref[i, 6:7, :] = carry_ref[2, pl.ds(groups[i], 1), :]
        total = now[128 * i : 128 * i + 128] + one_ref[i, 7:135, :] + two_ref[i, 6:134, :]
        mix_ref[i, pl.ds(0, 128, stride=2), :] = total[:, :128]
        mix_ref[i, pl.ds(1, 128, stride=2), :] = total[:, 128:]
        outs.append(mix_ref[i].astype(BF))
    return outs


def exchange_kernel(
    x_parts, z_parts, y_parts, c_parts,
    order_ref, live_ref, volt_ref, table_ref, beam_ref, taps_ref, coef_ref,
    early_ref, last_ref, filt_out_ref, carry_out_ref,
    perm, hot, stack, weight, sorted_volt, rows, send, recv0, recv1, recv2, recv3, filt, edge, edge_send, edge_recv, carry,
    one, two, mix, stage,
    send_sem, recv_sem, edge_sem, edge_recv_sem, out_sem,
):
    recv = (recv0, recv1, recv2, recv3)
    me = lax.axis_index("sub")
    half = lax.axis_index("tm")
    devices = x_parts * z_parts * y_parts * c_parts
    slots = volt_ref.shape[0]
    live = live_ref[0]

    barrier = pltpu.get_barrier_semaphore()

    def greet(i, _):
        @pl.when(i != me)
        def _():
            pl.semaphore_signal(barrier, inc=1, device_id=(i, half), device_id_type=MESH)
        return 0

    lax.fori_loop(0, devices, greet, 0)
    pl.semaphore_signal(barrier, inc=1, device_id=(me, 1 - half), device_id_type=MESH)

    for b in range(4):
        row = iota((128, 256), 0)
        pick = iota((128, 256), 1) == 4 * (row // 2) + b
        key = jnp.sum(
            jnp.where(pick, jnp.broadcast_to(beam_ref[...].astype(F32), (128, 256)), 0.0), axis=1, keepdims=True
        )
        key = key.astype(jnp.int32) + 384 * (iota((128, 1), 0) % 2)
        hot[128 * b : 128 * b + 128, :] = (iota((128, 768), 1) == key).astype(F32).astype(BF)
    def fill(i, _):
        ahead = iota((128, 128), 0) + 128 * i - 8 * iota((128, 128), 1)
        for t in range(8):
            perm[pl.ds(pl.multiple_of(128 * i, 128), 128), 128 * t : 128 * t + 128] = (ahead == t).astype(F32).astype(BF)
        return 0

    lax.fori_loop(0, 8, fill, 0)
    stack[...] = jnp.zeros_like(stack)

    def prepare(s, _):
        real, imag = table_ref[s, 0], table_ref[s, 1]
        stack[0:96, 0:320] = real
        stack[0:96, 384:704] = imag
        stack[96:192, 0:320] = -imag
        stack[96:192, 384:704] = real
        weight[s] = lax.dot_general(hot[...], stack[...], NT, preferred_element_type=F32).astype(BF)
        for n in range(4):
            sorted_volt[s, :, 256 * n : 256 * n + 256] = jnp.dot(
                volt_ref[s], perm[:, 256 * n : 256 * n + 256], preferred_element_type=F32
            ).astype(BF)
        return 0

    lax.fori_loop(0, slots, prepare, 0)
    pl.semaphore_wait(barrier, devices)

    def peer(dx, dz, dy, dc):
        c = me % c_parts
        y = (me // c_parts) % y_parts
        z = (me // (c_parts * y_parts)) % z_parts
        x = me // (c_parts * y_parts * z_parts)
        return (
            ((x + dx) % x_parts * z_parts + (z + dz) % z_parts) * y_parts + (y + dy) % y_parts
        ) * c_parts + (c + dc) % c_parts

    part = slots // 2

    def pair(b, k):
        h, j = k // 32, k % 32
        dy = j % y_parts
        dz = (j // y_parts) % z_parts
        dc = j // (y_parts * z_parts)
        far = peer(1, dz, dy, dc)
        near = peer(0, dz + z_parts // 2, dy + y_parts // 2, dc)

        def copy(target, i):
            return pltpu.make_async_remote_copy(
                src_ref=send.at[b, target, pl.ds(h * part, part)],
                dst_ref=recv[b].at[pl.ds(me * slots + h * part, part)],
                send_sem=send_sem.at[i, j],
                recv_sem=recv_sem.at[b],
                device_id=(target, half),
                device_id_type=MESH,
            )

        return copy(far, 0), copy(near, 1), near != me

    def ship(b, k, first=False):
        far, near, apart = pair(b, k)
        if not first:
            far.wait_send()
        far.start()

        @pl.when(apart)
        def _():
            if not first:
                near.wait_send()
            near.start()

    def ship_range(b, lo, hi, first=False):
        def step(k, _):
            ship(b, k, first)
            return 0

        lax.fori_loop(lo, hi, step, 0)

    def form_beam(b):
        def form(s, _):
            for n in range(4):
                out = jnp.dot(
                    weight[s, 128 * b : 128 * b + 128, :],
                    sorted_volt[s, :, 256 * n : 256 * n + 256],
                    preferred_element_type=F32,
                )
                rows[pl.ds(2 * n, 128, stride=8), :] = out[:, :128]
                rows[pl.ds(2 * n + 1, 128, stride=8), :] = out[:, 128:]
            send[b, :, s] = rows[...].astype(BF).reshape(devices, 16, 128)
            return 0

        lax.fori_loop(0, slots, form, 0)
        recv[b][pl.ds(me * slots, slots)] = send[b, me]

    form_beam(0)
    ship_range(0, 0, 32, first=True)
    for b in range(1, 4):
        form_beam(b)
    build_filter(taps_ref, coef_ref, filt)
    save_filter = pltpu.make_async_copy(filt, filt_out_ref, out_sem.at[0])
    save_filter.start()

    ship_range(0, 32, 64)
    ship_range(1, 0, 32)

    def arrived(b):
        blocks = (devices - 1) * slots
        pltpu.make_async_remote_copy(
            src_ref=recv[b].at[pl.ds(0, blocks)],
            dst_ref=recv[b].at[pl.ds(0, blocks)],
            send_sem=send_sem.at[0, 0],
            recv_sem=recv_sem.at[b],
            device_id=(me, 1 - half),
            device_id_type=MESH,
        ).wait_recv()

    tail = (iota((16, 128), 1) == iota((16, 128), 0) + 112).astype(F32).astype(BF)
    pending = None
    for b in range(4):
        arrived(b)
        if b == 3:
            save_last = pltpu.make_async_copy(recv[3], last_ref, out_sem.at[2])
            save_last.start()

        def cut(i, _):
            for u in range(3):
                g = 3 * i + u
                ends = lax.dot_general(tail, band(recv[b], order_ref, live, g), NT, preferred_element_type=F32)
                edge[0, pl.ds(g, 1), :] = ends[15:16]
                edge[1, pl.ds(g, 1), :] = ends[14:15]
            if b < 3:
                for u in range(2):
                    ship(b + 1, 32 + 2 * i + u)
            return 0

        lax.fori_loop(0, 16, cut, 0)
        edge_send[b] = edge[...].astype(BF)
        edges = pltpu.make_async_remote_copy(
            src_ref=edge_send.at[b],
            dst_ref=edge_recv.at[b],
            send_sem=edge_sem.at[b],
            recv_sem=edge_recv_sem.at[b],
            device_id=(me, 1 - half),
            device_id_type=MESH,
        )
        edges.start()
        edges.wait()
        keep = jnp.where(half == 1, 1.0, 0.0).astype(F32)
        near, far = edge_recv[b, 0], edge_recv[b, 1]
        carry[0] = keep * jnp.dot(near, filt[1], preferred_element_type=F32)
        carry[1] = keep * jnp.dot(near, filt[2], preferred_element_type=F32)
        carry[2] = keep * jnp.dot(far, filt[2], preferred_element_type=F32)
        if b < EARLY:
            if pending is not None:
                pending.wait()

            def make(i, _):
                gs = [3 * i + u for u in range(3)]
                bands = [band(recv[b], order_ref, live, g) for g in gs]
                for g, y in zip(gs, synthesise(bands, gs, carry, filt, one, two, mix)):
                    stage[g] = y
                return 0

            lax.fori_loop(0, 16, make, 0)
            pending = pltpu.make_async_copy(stage, early_ref.at[b], out_sem.at[1])
            pending.start()
            if b < 2:
                ship_range(b + 2, 0, 32)
    save_carry = pltpu.make_async_copy(carry, carry_out_ref, out_sem.at[3])
    save_carry.start()

    def drain(k, _):
        far, near, apart = pair(3, 32 + k)
        far.wait_send()

        @pl.when(apart)
        def _():
            near.wait_send()
        return 0

    lax.fori_loop(0, 32, drain, 0)
    pending.wait()
    save_filter.wait()
    save_last.wait()
    save_carry.wait()


def finish_kernel(order_ref, live_ref, early_ref, last_ref, filt_ref, carry_ref, out_ref, one, two, mix):
    i = pl.program_id(0)
    b = i % 4
    first = (i // 4) * 8

    @pl.when(b < EARLY)
    def _():
        out_ref[...] = early_ref[...]

    @pl.when(b == EARLY)
    def _():
        live = live_ref[0]

        def make(k, _):
            at = [4 * k + u for u in range(4)]
            bands = [band(last_ref, order_ref, live, first + n) for n in at]
            ys = synthesise(bands, [first + n for n in at], carry_ref, filt_ref, one, two, mix)
            for n, y in zip(at, ys):
                out_ref[0, n] = y
            return 0

        lax.fori_loop(0, 2, make, 0)


def on_device(sizes, voltages, pointing_table, beam_pointing, subband_order, live_subbands, filter_taps):
    slots = voltages.shape[0]
    devices = sizes[0] * sizes[1] * sizes[2] * sizes[3]
    volt = voltages.reshape(slots, 192, 1024)
    table = jnp.swapaxes(pointing_table, 2, 3)
    beams = beam_pointing.reshape(1, 256)
    coef = jnp.asarray(coefficient_rows())
    smem = pl.BlockSpec(memory_space=pltpu.SMEM)
    vmem = pl.BlockSpec(memory_space=pltpu.VMEM)
    hbm = pl.BlockSpec(memory_space=pl.ANY)
    VM = pltpu.VMEM
    def synth_scratch(n):
        return [VM((n, 136, 256), F32), VM((n, 136, 256), F32), VM((n, 256, 128), F32)]

    early, last, filt, carry = pl.pallas_call(
        functools.partial(exchange_kernel, *sizes),
        name="exchange",
        out_shape=[
            jax.ShapeDtypeStruct((EARLY, 48, 256, 128), BF),
            jax.ShapeDtypeStruct((devices * slots, 16, 128), BF),
            jax.ShapeDtypeStruct((3, 256, 256), BF),
            jax.ShapeDtypeStruct((3, 48, 256), F32),
        ],
        in_specs=[smem, smem, vmem, vmem, vmem, vmem, vmem],
        out_specs=[hbm] * 4,
        scratch_shapes=[
            VM((1024, 1024), BF),
            VM((512, 768), BF),
            VM((192, 768), BF),
            VM((slots, 512, 192), BF),
            VM((slots, 192, 1024), BF),
            VM((1024, 128), F32),
            VM((4, devices, slots, 16, 128), BF),
            *[VM((devices * slots, 16, 128), BF)] * 4,
            VM((3, 256, 256), BF),
            VM((2, 48, 256), F32),
            VM((4, 2, 48, 256), BF),
            VM((4, 2, 48, 256), BF),
            VM((3, 48, 256), F32),
            *synth_scratch(3),
            VM((48, 256, 128), BF),
            pltpu.SemaphoreType.DMA((2, 32)),
            pltpu.SemaphoreType.DMA((4,)),
            pltpu.SemaphoreType.DMA((4,)),
            pltpu.SemaphoreType.DMA((4,)),
            pltpu.SemaphoreType.DMA((4,)),
        ],
        compiler_params=pltpu.CompilerParams(
            collective_id=0, has_side_effects=True, vmem_limit_bytes=62 * 1024 * 1024
        ),
    )(subband_order, live_subbands, volt, table, beams, filter_taps, coef)

    out = pl.pallas_call(
        finish_kernel,
        name="finish",
        grid=(24,),
        out_shape=jax.ShapeDtypeStruct((4, 48, 256, 128), BF),
        in_specs=[
            smem,
            smem,
            pl.BlockSpec((1, 8, 256, 128), lambda i: (jnp.minimum(i % 4, EARLY - 1), i // 4, 0, 0)),
            pl.BlockSpec((devices * slots, 16, 128), lambda i: (0, 0, 0)),
            pl.BlockSpec((3, 256, 256), lambda i: (0, 0, 0)),
            pl.BlockSpec((3, 48, 256), lambda i: (0, 0, 0)),
        ],
        out_specs=pl.BlockSpec((1, 8, 256, 128), lambda i: (i % 4, i // 4, 0, 0)),
        scratch_shapes=synth_scratch(4),
        compiler_params=pltpu.CompilerParams(vmem_limit_bytes=60 * 1024 * 1024),
    )(subband_order, live_subbands, early, last, filt, carry)
    out = out.reshape(4, 48, 128, 2, 128)
    return jnp.swapaxes(out, 2, 3).reshape(4, 48, 2, 16384)


def solution(mesh):
    sizes = (2, 4, 4, 2)
    in_specs = (P("sub", None, None, "tm"), P("sub", None, None, None), P(), P(), P(), P())
    out_specs = P("sub", None, None, "tm")
    return jax.shard_map(
        functools.partial(on_device, sizes), mesh=mesh, in_specs=in_specs, out_specs=out_specs, check_vma=False
    )
```

```python
import functools

import jax
import jax.numpy as jnp
import numpy as np
from jax import lax
from jax.experimental import pallas as pl
from jax.experimental.pallas import tpu as pltpu
from jax.sharding import PartitionSpec as P

MESH = pl.DeviceIdType.MESH
BF = jnp.bfloat16
F32 = jnp.float32
NT = (((1,), (1,)), ((), ()))
EARLY = 3


def coefficient_rows():
    k = np.arange(16)
    phase = ((np.outer(k, k) % 16).astype(np.float32) * np.float32(2.0 * np.pi / 16)).astype(np.float32)
    cos = np.cos(phase).astype(jnp.bfloat16).astype(np.float32)
    sin = np.sin(phase).astype(jnp.bfloat16).astype(np.float32)
    rows = np.stack([np.stack([cos, -sin]), np.stack([sin, cos])])
    rows = rows.transpose(0, 1, 3, 2).reshape(64, 16)
    return np.tile(rows, (1, 8)).astype(np.float32)


def iota(shape, dim):
    return lax.broadcasted_iota(jnp.int32, shape, dim)


def build_filter(taps_ref, coef_ref, filt_ref):
    repeat = (iota((16, 128), 1) % 16 == iota((16, 128), 0)).astype(F32)
    taps = jnp.dot(taps_ref[...], repeat, precision=lax.Precision.HIGHEST, preferred_element_type=F32)
    lag = iota((8, 128), 1) // 16 - iota((8, 128), 0)
    for d in range(3):
        tap = jnp.zeros((8, 128), F32)
        for j in range(16):
            tap = jnp.where(lag + 8 * d == j, jnp.broadcast_to(taps[j : j + 1], (8, 128)), tap)
        for q in range(2):
            for c in range(16):
                block = [
                    tap * coef_ref[(2 * q + p) * 16 + c : (2 * q + p) * 16 + c + 1, :] for p in range(2)
                ]
                filt_ref[d, 16 * c : 16 * c + 16, 128 * q : 128 * q + 128] = jnp.concatenate(
                    block, axis=0
                ).astype(BF)


def band(rows_ref, order_ref, live, group):
    parts = []
    for c in range(16):
        f = group * 16 + c
        part = rows_ref[order_ref[f]]
        parts.append(jnp.where(f < live, part, jnp.zeros_like(part)))
    return jnp.concatenate(parts, axis=0)


def synthesise(bands, groups, carry_ref, filt_ref, one_ref, two_ref, mix_ref):
    n = len(bands)
    zt = jnp.concatenate([z.T for z in bands], axis=0)
    now = jnp.dot(zt, filt_ref[0], preferred_element_type=F32)
    one = jnp.dot(zt, filt_ref[1], preferred_element_type=F32)
    two = jnp.dot(zt, filt_ref[2], preferred_element_type=F32)
    outs = []
    for i in range(n):
        one_ref[i, 8:136, :] = one[128 * i : 128 * i + 128]
        two_ref[i, 8:136, :] = two[128 * i : 128 * i + 128]
        one_ref[i, 7:8, :] = carry_ref[0, pl.ds(groups[i], 1), :]
        two_ref[i, 7:8, :] = carry_ref[1, pl.ds(groups[i], 1), :]
        two_ref[i, 6:7, :] = carry_ref[2, pl.ds(groups[i], 1), :]
        total = now[128 * i : 128 * i + 128] + one_ref[i, 7:135, :] + two_ref[i, 6:134, :]
        mix_ref[i, pl.ds(0, 128, stride=2), :] = total[:, :128]
        mix_ref[i, pl.ds(1, 128, stride=2), :] = total[:, 128:]
        outs.append(mix_ref[i].astype(BF))
    return outs


def exchange_kernel(
    x_parts, z_parts, y_parts, c_parts,
    order_ref, live_ref, volt_ref, table_ref, beam_ref, taps_ref, coef_ref,
    early_ref, last_ref, filt_out_ref, carry_out_ref,
    volt, perm, hot, stack, sorted_volt, rows, send, recv0, recv1, recv2, recv3, filt, edge, edge_send, edge_recv, carry,
    one, two, mix, stage,
    send_sem, recv_sem, edge_sem, edge_recv_sem, out_sem, load_sem,
):
    recv = (recv0, recv1, recv2, recv3)
    me = lax.axis_index("sub")
    half = lax.axis_index("tm")
    devices = x_parts * z_parts * y_parts * c_parts
    slots = volt_ref.shape[0]
    live = live_ref[0]

    barrier = pltpu.get_barrier_semaphore()

    def greet(i, _):
        @pl.when(i != me)
        def _():
            pl.semaphore_signal(barrier, inc=1, device_id=(i, half), device_id_type=MESH)
        return 0

    lax.fori_loop(0, devices, greet, 0)
    pl.semaphore_signal(barrier, inc=1, device_id=(me, 1 - half), device_id_type=MESH)

    load = [
        pltpu.make_async_copy(volt_ref.at[pl.ds(6 * h, 6)], volt.at[pl.ds(6 * h, 6)], load_sem.at[h])
        for h in range(2)
    ]
    for copy in load:
        copy.start()
    for b in range(4):
        row = iota((128, 256), 0)
        pick = iota((128, 256), 1) == 4 * (row // 2) + b
        key = jnp.sum(
            jnp.where(pick, jnp.broadcast_to(beam_ref[...].astype(F32), (128, 256)), 0.0), axis=1, keepdims=True
        )
        key = key.astype(jnp.int32) + 384 * (iota((128, 1), 0) % 2)
        hot[128 * b : 128 * b + 128, :] = (iota((128, 768), 1) == key).astype(F32).astype(BF)
    def fill(i, _):
        ahead = iota((128, 128), 0) + 128 * i - 8 * iota((128, 128), 1)
        for t in range(8):
            perm[pl.ds(pl.multiple_of(128 * i, 128), 128), 128 * t : 128 * t + 128] = (ahead == t).astype(F32).astype(BF)
        return 0

    lax.fori_loop(0, 8, fill, 0)
    stack[...] = jnp.zeros_like(stack)
    part = slots // 2

    def peer(dx, dz, dy, dc):
        c = me % c_parts
        y = (me // c_parts) % y_parts
        z = (me // (c_parts * y_parts)) % z_parts
        x = me // (c_parts * y_parts * z_parts)
        return (
            ((x + dx) % x_parts * z_parts + (z + dz) % z_parts) * y_parts + (y + dy) % y_parts
        ) * c_parts + (c + dc) % c_parts

    def pair(b, k):
        h, j = k // 32, k % 32
        dy = j % y_parts
        dz = (j // y_parts) % z_parts
        dc = j // (y_parts * z_parts)
        far = peer(1, dz, dy, dc)
        near = peer(0, dz + z_parts // 2, dy + y_parts // 2, dc)

        def copy(target, i):
            return pltpu.make_async_remote_copy(
                src_ref=send.at[b, target, pl.ds(h * part, part)],
                dst_ref=recv[b].at[pl.ds(me * slots + h * part, part)],
                send_sem=send_sem.at[i, k],
                recv_sem=recv_sem.at[b],
                device_id=(target, half),
                device_id_type=MESH,
            )

        return copy(far, 0), copy(near, 1), near != me

    def ship(b, k, first=False):
        far, near, apart = pair(b, k)
        if not first:
            far.wait_send()
        far.start()

        @pl.when(apart)
        def _():
            if not first:
                near.wait_send()
            near.start()

    def ship_range(b, lo, hi, first=False):
        def step(k, _):
            ship(b, k, first)
            return 0

        lax.fori_loop(lo, hi, step, 0)

    def sort(s, _):
        for n in range(4):
            sorted_volt[s, :, 256 * n : 256 * n + 256] = jnp.dot(
                volt[s], perm[:, 256 * n : 256 * n + 256], preferred_element_type=F32
            ).astype(BF)
        return 0

    def form_beam(b, lo, hi):
        def form(s, _):
            real, imag = table_ref[s, 0], table_ref[s, 1]
            stack[0:96, 0:320] = real
            stack[0:96, 384:704] = imag
            stack[96:192, 0:320] = -imag
            stack[96:192, 384:704] = real
            weight = lax.dot_general(
                hot[128 * b : 128 * b + 128, :], stack[...], NT, preferred_element_type=F32
            ).astype(BF)
            for n in range(4):
                out = jnp.dot(
                    weight, sorted_volt[s, :, 256 * n : 256 * n + 256], preferred_element_type=F32
                )
                rows[pl.ds(2 * n, 128, stride=8), :] = out[:, :128]
                rows[pl.ds(2 * n + 1, 128, stride=8), :] = out[:, 128:]
            send[b, :, s] = rows[...].astype(BF).reshape(devices, 16, 128)
            return 0

        lax.fori_loop(lo, hi, form, 0)
        recv[b][pl.ds(me * slots + lo, hi - lo)] = send[b, me, lo:hi]

    for h in range(2):
        load[h].wait()
        lax.fori_loop(part * h, part * h + part, sort, 0)
        form_beam(0, part * h, part * h + part)
        if h == 0:
            pl.semaphore_wait(barrier, devices)
        ship_range(0, 32 * h, 32 * h + 32, first=True)
    for b in range(1, 4):
        form_beam(b, 0, slots)
    build_filter(taps_ref, coef_ref, filt)
    save_filter = pltpu.make_async_copy(filt, filt_out_ref, out_sem.at[0])
    save_filter.start()

    ship_range(1, 0, 64)

    def arrived(b):
        blocks = (devices - 1) * slots
        pltpu.make_async_remote_copy(
            src_ref=recv[b].at[pl.ds(0, blocks)],
            dst_ref=recv[b].at[pl.ds(0, blocks)],
            send_sem=send_sem.at[0, 0],
            recv_sem=recv_sem.at[b],
            device_id=(me, 1 - half),
            device_id_type=MESH,
        ).wait_recv()

    tail = (iota((16, 128), 1) == iota((16, 128), 0) + 112).astype(F32).astype(BF)
    pending = None
    for b in range(4):
        arrived(b)
        if b == 3:
            save_last = pltpu.make_async_copy(recv[3], last_ref, out_sem.at[2])
            save_last.start()

        def cut(i, _):
            for u in range(3):
                g = 3 * i + u
                ends = lax.dot_general(tail, band(recv[b], order_ref, live, g), NT, preferred_element_type=F32)
                edge[0, pl.ds(g, 1), :] = ends[15:16]
                edge[1, pl.ds(g, 1), :] = ends[14:15]
            if b < 2:
                for u in range(2):
                    ship(b + 2, 2 * i + u)
            return 0

        lax.fori_loop(0, 16, cut, 0)
        edge_send[b] = edge[...].astype(BF)
        edges = pltpu.make_async_remote_copy(
            src_ref=edge_send.at[b],
            dst_ref=edge_recv.at[b],
            send_sem=edge_sem.at[b],
            recv_sem=edge_recv_sem.at[b],
            device_id=(me, 1 - half),
            device_id_type=MESH,
        )
        edges.start()
        edges.wait()
        keep = jnp.where(half == 1, 1.0, 0.0).astype(F32)
        near, far = edge_recv[b, 0], edge_recv[b, 1]
        carry[0] = keep * jnp.dot(near, filt[1], preferred_element_type=F32)
        carry[1] = keep * jnp.dot(near, filt[2], preferred_element_type=F32)
        carry[2] = keep * jnp.dot(far, filt[2], preferred_element_type=F32)
        if b < EARLY:
            if pending is not None:
                pending.wait()

            def make(i, _):
                gs = [3 * i + u for u in range(3)]
                bands = [band(recv[b], order_ref, live, g) for g in gs]
                for g, y in zip(gs, synthesise(bands, gs, carry, filt, one, two, mix)):
                    stage[g] = y
                if b < 2:
                    for u in range(2):
                        ship(b + 2, 32 + 2 * i + u)
                return 0

            lax.fori_loop(0, 16, make, 0)
            pending = pltpu.make_async_copy(stage, early_ref.at[b], out_sem.at[1])
            pending.start()
    save_carry = pltpu.make_async_copy(carry, carry_out_ref, out_sem.at[3])
    save_carry.start()

    def drain(k, _):
        far, near, apart = pair(3, k)
        far.wait_send()

        @pl.when(apart)
        def _():
            near.wait_send()
        return 0

    lax.fori_loop(0, 64, drain, 0)
    pending.wait()
    save_filter.wait()
    save_last.wait()
    save_carry.wait()


def finish_kernel(
    order_ref, live_ref, early_ref, last_ref, filt_ref, carry_ref, out_ref,
    last, filt, carry, early, stage, one, two, mix, small_sem, in_sem, out_sem, stage_sem,
):
    small = [
        pltpu.make_async_copy(last_ref, last, small_sem.at[0]),
        pltpu.make_async_copy(filt_ref, filt, small_sem.at[1]),
        pltpu.make_async_copy(carry_ref, carry, small_sem.at[2]),
    ]
    for copy in small:
        copy.start()
    count = early.shape[0] // 12

    def take(i):
        return pltpu.make_async_copy(early_ref.at[pl.ds(count * i, count)], early.at[pl.ds(count * i, count)], in_sem.at[i])

    def give(i):
        return pltpu.make_async_copy(early.at[pl.ds(count * i, count)], out_ref.at[pl.ds(count * i, count)], out_sem.at[i])

    def put(i):
        return pltpu.make_async_copy(
            stage.at[pl.ds(4 * i, 4)], out_ref.at[pl.ds(48 * EARLY + 4 * i, 4)], stage_sem.at[i]
        )

    for i in range(12):
        take(i).start()
    for copy in small:
        copy.wait()
    live = live_ref[0]

    def make(i, _):
        gs = [4 * i + u for u in range(4)]
        bands = [band(last, order_ref, live, g) for g in gs]
        for g, y in zip(gs, synthesise(bands, gs, carry, filt, one, two, mix)):
            stage[g] = y
        take(i).wait()
        give(i).start()
        put(i).start()
        return 0

    lax.fori_loop(0, 12, make, 0)

    def close(i, _):
        give(i).wait()
        put(i).wait()
        return 0

    lax.fori_loop(0, 12, close, 0)


def on_device(sizes, voltages, pointing_table, beam_pointing, subband_order, live_subbands, filter_taps):
    slots = voltages.shape[0]
    devices = sizes[0] * sizes[1] * sizes[2] * sizes[3]
    volt = voltages.reshape(slots, 192, 1024)
    table = jnp.swapaxes(pointing_table, 2, 3)
    beams = beam_pointing.reshape(1, 256)
    coef = jnp.asarray(coefficient_rows())
    smem = pl.BlockSpec(memory_space=pltpu.SMEM)
    vmem = pl.BlockSpec(memory_space=pltpu.VMEM)
    hbm = pl.BlockSpec(memory_space=pl.ANY)
    VM = pltpu.VMEM
    def synth_scratch(n):
        return [VM((n, 136, 256), F32), VM((n, 136, 256), F32), VM((n, 256, 128), F32)]

    early, last, filt, carry = pl.pallas_call(
        functools.partial(exchange_kernel, *sizes),
        name="exchange",
        out_shape=[
            jax.ShapeDtypeStruct((EARLY, 48, 256, 128), BF),
            jax.ShapeDtypeStruct((devices * slots, 16, 128), BF),
            jax.ShapeDtypeStruct((3, 256, 256), BF),
            jax.ShapeDtypeStruct((3, 48, 256), F32),
        ],
        in_specs=[smem, smem, hbm, vmem, vmem, vmem, vmem],
        out_specs=[hbm] * 4,
        scratch_shapes=[
            VM((slots, 192, 1024), BF),
            VM((1024, 1024), BF),
            VM((512, 768), BF),
            VM((192, 768), BF),
            VM((slots, 192, 1024), BF),
            VM((1024, 128), F32),
            VM((4, devices, slots, 16, 128), BF),
            *[VM((devices * slots, 16, 128), BF)] * 4,
            VM((3, 256, 256), BF),
            VM((2, 48, 256), F32),
            VM((4, 2, 48, 256), BF),
            VM((4, 2, 48, 256), BF),
            VM((3, 48, 256), F32),
            *synth_scratch(3),
            VM((48, 256, 128), BF),
            pltpu.SemaphoreType.DMA((2, 64)),
            pltpu.SemaphoreType.DMA((4,)),
            pltpu.SemaphoreType.DMA((4,)),
            pltpu.SemaphoreType.DMA((4,)),
            pltpu.SemaphoreType.DMA((4,)),
            pltpu.SemaphoreType.DMA((2,)),
        ],
        compiler_params=pltpu.CompilerParams(
            collective_id=0, has_side_effects=True, vmem_limit_bytes=62 * 1024 * 1024
        ),
    )(subband_order, live_subbands, volt, table, beams, filter_taps, coef)

    out = pl.pallas_call(
        finish_kernel,
        name="finish",
        out_shape=jax.ShapeDtypeStruct((192, 256, 128), BF),
        in_specs=[smem, smem, hbm, hbm, hbm, hbm],
        out_specs=hbm,
        scratch_shapes=[
            VM((devices * slots, 16, 128), BF),
            VM((3, 256, 256), BF),
            VM((3, 48, 256), F32),
            VM((48 * EARLY, 256, 128), BF),
            VM((48, 256, 128), BF),
            *synth_scratch(4),
            pltpu.SemaphoreType.DMA((3,)),
            pltpu.SemaphoreType.DMA((12,)),
            pltpu.SemaphoreType.DMA((12,)),
            pltpu.SemaphoreType.DMA((12,)),
        ],
        compiler_params=pltpu.CompilerParams(vmem_limit_bytes=60 * 1024 * 1024),
    )(subband_order, live_subbands, early.reshape(48 * EARLY, 256, 128), last, filt, carry)
    out = out.reshape(4, 48, 128, 2, 128)
    return jnp.swapaxes(out, 2, 3).reshape(4, 48, 2, 16384)


def solution(mesh):
    sizes = (2, 4, 4, 2)
    in_specs = (P("sub", None, None, "tm"), P("sub", None, None, None), P(), P(), P(), P())
    out_specs = P("sub", None, None, "tm")
    return jax.shard_map(
        functools.partial(on_device, sizes), mesh=mesh, in_specs=in_specs, out_specs=out_specs, check_vma=False
    )
```

```python
import functools

import jax
import jax.numpy as jnp
import numpy as np
from jax import lax
from jax.experimental import pallas as pl
from jax.experimental.pallas import tpu as pltpu
from jax.sharding import PartitionSpec as P

MESH = pl.DeviceIdType.MESH
BF = jnp.bfloat16
F32 = jnp.float32
NT = (((1,), (1,)), ((), ()))
EARLY = 3


def coefficient_rows():
    k = np.arange(16)
    phase = ((np.outer(k, k) % 16).astype(np.float32) * np.float32(2.0 * np.pi / 16)).astype(np.float32)
    cos = np.cos(phase).astype(jnp.bfloat16).astype(np.float32)
    sin = np.sin(phase).astype(jnp.bfloat16).astype(np.float32)
    rows = np.stack([np.stack([cos, -sin]), np.stack([sin, cos])])
    rows = rows.transpose(0, 1, 3, 2).reshape(64, 16)
    return np.tile(rows, (1, 8)).astype(np.float32)


def iota(shape, dim):
    return lax.broadcasted_iota(jnp.int32, shape, dim)


def build_filter(taps_ref, coef_ref, filt_ref):
    repeat = (iota((16, 128), 1) % 16 == iota((16, 128), 0)).astype(F32)
    taps = jnp.dot(taps_ref[...], repeat, precision=lax.Precision.HIGHEST, preferred_element_type=F32)
    lag = iota((8, 128), 1) // 16 - iota((8, 128), 0)
    for d in range(3):
        tap = jnp.zeros((8, 128), F32)
        for j in range(16):
            tap = jnp.where(lag + 8 * d == j, jnp.broadcast_to(taps[j : j + 1], (8, 128)), tap)
        for q in range(2):
            for c in range(16):
                block = [
                    tap * coef_ref[(2 * q + p) * 16 + c : (2 * q + p) * 16 + c + 1, :] for p in range(2)
                ]
                filt_ref[d, 16 * c : 16 * c + 16, 128 * q : 128 * q + 128] = jnp.concatenate(
                    block, axis=0
                ).astype(BF)


def band(rows_ref, order_ref, live, group, gap=0):
    parts = []
    for c in range(16):
        f = group * 16 + c
        slot = order_ref[f]
        part = rows_ref[slot + slot // gap if gap else slot]
        parts.append(jnp.where(f < live, part, jnp.zeros_like(part)))
    return jnp.concatenate(parts, axis=0)


def synthesise(bands, groups, carry_ref, filt_ref, one_ref, two_ref, mix_ref):
    n = len(bands)
    zt = jnp.concatenate([z.T for z in bands], axis=0)
    now = jnp.dot(zt, filt_ref[0], preferred_element_type=F32)
    one = jnp.dot(zt, filt_ref[1], preferred_element_type=F32)
    two = jnp.dot(zt, filt_ref[2], preferred_element_type=F32)
    outs = []
    for i in range(n):
        one_ref[i, 8:136, :] = one[128 * i : 128 * i + 128]
        two_ref[i, 8:136, :] = two[128 * i : 128 * i + 128]
        one_ref[i, 7:8, :] = carry_ref[0, pl.ds(groups[i], 1), :]
        two_ref[i, 7:8, :] = carry_ref[1, pl.ds(groups[i], 1), :]
        two_ref[i, 6:7, :] = carry_ref[2, pl.ds(groups[i], 1), :]
        total = now[128 * i : 128 * i + 128] + one_ref[i, 7:135, :] + two_ref[i, 6:134, :]
        mix_ref[i, pl.ds(0, 128, stride=2), :] = total[:, :128]
        mix_ref[i, pl.ds(1, 128, stride=2), :] = total[:, 128:]
        outs.append(mix_ref[i].astype(BF))
    return outs


def exchange_kernel(
    x_parts, z_parts, y_parts, c_parts,
    order_ref, live_ref, volt_ref, table_ref, beam_ref, taps_ref, coef_ref,
    early_ref, last_ref, filt_out_ref, carry_out_ref,
    volt, perm, hot, stack, sorted_volt, rows, send, recv0, recv1, recv2, recv3, filt, ends, edge, tail_send, tail_recv, picked, carry,
    one, two, mix, stage,
    send_sem, recv_sem, edge_sem, out_sem, load_sem,
):
    recv = (recv0, recv1, recv2, recv3)
    me = lax.axis_index("sub")
    half = lax.axis_index("tm")
    devices = x_parts * z_parts * y_parts * c_parts
    slots = volt_ref.shape[0]
    live = live_ref[0]
    width = (slots, slots + 1, slots, slots)

    barrier = pltpu.get_barrier_semaphore()

    tail_recv[...] = jnp.zeros_like(tail_recv)
    ends[...] = jnp.zeros_like(ends)

    def greet(i, _):
        @pl.when(i != me)
        def _():
            pl.semaphore_signal(barrier, inc=1, device_id=(i, half), device_id_type=MESH)

        return 0

    lax.fori_loop(0, devices, greet, 0)
    pl.semaphore_signal(barrier, inc=1, device_id=(me, 1 - half), device_id_type=MESH)

    load = [
        pltpu.make_async_copy(volt_ref.at[pl.ds(6 * h, 6)], volt.at[pl.ds(6 * h, 6)], load_sem.at[h])
        for h in range(2)
    ]
    for copy in load:
        copy.start()
    for b in range(4):
        row = iota((128, 256), 0)
        pick = iota((128, 256), 1) == 4 * (row // 2) + b
        key = jnp.sum(
            jnp.where(pick, jnp.broadcast_to(beam_ref[...].astype(F32), (128, 256)), 0.0), axis=1, keepdims=True
        )
        key = key.astype(jnp.int32) + 384 * (iota((128, 1), 0) % 2)
        hot[128 * b : 128 * b + 128, :] = (iota((128, 768), 1) == key).astype(F32).astype(BF)
    def fill(i, _):
        ahead = iota((128, 128), 0) + 128 * i - 8 * iota((128, 128), 1)
        for t in range(8):
            perm[pl.ds(pl.multiple_of(128 * i, 128), 128), 128 * t : 128 * t + 128] = (ahead == t).astype(F32).astype(BF)
        return 0

    lax.fori_loop(0, 8, fill, 0)
    stack[...] = jnp.zeros_like(stack)
    part = slots // 2

    def peer(dx, dz, dy, dc):
        c = me % c_parts
        y = (me // c_parts) % y_parts
        z = (me // (c_parts * y_parts)) % z_parts
        x = me // (c_parts * y_parts * z_parts)
        return (
            ((x + dx) % x_parts * z_parts + (z + dz) % z_parts) * y_parts + (y + dy) % y_parts
        ) * c_parts + (c + dc) % c_parts

    def pair(b, j, lo, count):
        dy = j % y_parts
        dz = (j // y_parts) % z_parts
        dc = j // (y_parts * z_parts)
        far = peer(1, dz, dy, dc)
        near = peer(0, dz + z_parts // 2, dy + y_parts // 2, dc)

        def copy(target, i):
            return pltpu.make_async_remote_copy(
                src_ref=send.at[b, target, pl.ds(lo, count)],
                dst_ref=recv[b].at[pl.ds(me * width[b] + lo, count)],
                send_sem=send_sem.at[i, b % 2, j],
                recv_sem=recv_sem.at[b],
                device_id=(target, half),
                device_id_type=MESH,
            )

        return copy(far, 0), copy(near, 1), near != me

    def ship(b, j, first, lo, count):
        far, near, apart = pair(b, j, lo, count)
        if not first:
            old_far, old_near, _ = pair(b - 2, j, 0, width[b - 2])
            old_far.wait_send()
        far.start()

        @pl.when(apart)
        def _():
            if not first:
                old_near.wait_send()
            near.start()

    def ship_range(b, lo, hi, first=False, slot=0, count=None):
        def step(j, _):
            ship(b, j, first, slot, width[b] if count is None else count)
            return 0

        lax.fori_loop(lo, hi, step, 0)

    def sort(s, _):
        for n in range(4):
            sorted_volt[s, :, 256 * n : 256 * n + 256] = jnp.dot(
                volt[s], perm[:, 256 * n : 256 * n + 256], preferred_element_type=F32
            ).astype(BF)
        return 0

    def weights(s, lo, hi):
        real, imag = table_ref[s, 0], table_ref[s, 1]
        stack[0:96, 0:320] = real
        stack[0:96, 384:704] = imag
        stack[96:192, 0:320] = -imag
        stack[96:192, 384:704] = real
        return lax.dot_general(hot[lo:hi, :], stack[...], NT, preferred_element_type=F32).astype(BF)

    def form_slot(b, s):
        weight = weights(s, 128 * b, 128 * b + 128)
        for n in range(4):
            out = jnp.dot(weight, sorted_volt[s, :, 256 * n : 256 * n + 256], preferred_element_type=F32)
            rows[pl.ds(2 * n, 128, stride=8), :] = out[:, :128]
            rows[pl.ds(2 * n + 1, 128, stride=8), :] = out[:, 128:]
        send[b, :, s] = rows[...].astype(BF).reshape(devices, 16, 128)

    def keep_own(b, lo, hi):
        recv[b][pl.ds(me * width[b] + lo, hi - lo)] = send[b, me, lo:hi]

    def form_beam(b):
        def form(s, _):
            form_slot(b, s)
            return 0

        lax.fori_loop(0, slots, form, 0)
        keep_own(b, 0, width[b])

    def begin(s, _):
        sort(s, 0)
        form_slot(0, s)
        return 0

    hand_on = pltpu.make_async_remote_copy(
        src_ref=tail_send,
        dst_ref=tail_recv,
        send_sem=edge_sem.at[0],
        recv_sem=edge_sem.at[1],
        device_id=(me, 1),
        device_id_type=MESH,
    )

    quarter = part // 2
    for lo, count, h in ((0, quarter, 0), (quarter, part - quarter, 0), (part, part, 1)):
        if lo == 0:
            load[0].wait()
        lax.fori_loop(lo, lo + count, begin, 0)
        keep_own(0, lo, lo + count)
        if lo == 0:
            pl.semaphore_wait(barrier, devices)
            load[1].wait()
            pick_tail = (iota((16, 128), 1) == iota((16, 128), 0) + 112).astype(F32).astype(BF)
            for s in range(slots):
                tail_send[s] = lax.dot_general(
                    pick_tail, volt[s, :, 896:1024], NT, preferred_element_type=F32
                ).astype(BF)

            @pl.when(half == 0)
            def _():
                hand_on.start()
        ship_range(0, 0, 32, True, lo, count)
    lane = iota((devices, 128), 1)

    def tails(s, _):
        ends[:, 0:16] = lax.dot_general(weights(s, 0, 512), tail_recv[s], NT, preferred_element_type=F32)
        total = jnp.zeros((devices, 128), F32)
        for b in range(4):
            for p in range(2):
                x = ends[pl.ds(128 * b + p, devices, stride=2), :]
                for e in range(2):
                    to = 32 * b + 16 * e + 8 * p
                    moved = pltpu.roll(x, (to - 8 * e) % 128, 1)
                    total = jnp.where((lane >= to) & (lane < to + 8), moved, total)
        edge[pl.ds(s, devices, stride=16), :] = total
        return 0

    @pl.when(half == 0)
    def _():
        hand_on.wait_send()

    @pl.when(half == 1)
    def _():
        hand_on.wait_recv()

    edge[...] = jnp.zeros_like(edge)
    lax.fori_loop(0, slots, tails, 0)
    send[1, :, slots] = edge[...].astype(BF).reshape(devices, 16, 128)
    form_beam(1)
    ship_range(1, 0, 32, True)
    form_beam(2)
    form_beam(3)
    ship_range(2, 0, 32)
    ship_range(3, 0, 32)
    build_filter(taps_ref, coef_ref, filt)
    save_filter = pltpu.make_async_copy(filt, filt_out_ref, out_sem.at[0])
    save_filter.start()

    def arrived(b):
        blocks = (devices - 1) * width[b]
        pltpu.make_async_remote_copy(
            src_ref=recv[b].at[pl.ds(0, blocks)],
            dst_ref=recv[b].at[pl.ds(0, blocks)],
            send_sem=send_sem.at[0, 0],
            recv_sem=recv_sem.at[b],
            device_id=(me, 1 - half),
            device_id_type=MESH,
        ).wait_recv()

    arrived(0)
    arrived(1)
    def unpack(d, _):
        edge[pl.ds(pl.multiple_of(16 * d, 16), 16), :] = recv[1][width[1] * d + slots].astype(F32)
        return 0

    lax.fori_loop(0, devices, unpack, 0)

    def pick(g, _):
        for c in range(16):
            f = 16 * g + c
            slot = order_ref[f]
            row = edge[pl.ds(slot + 4 * (slot // slots), 1), :]
            picked[pl.ds(f, 1), :] = jnp.where(f < live, row, jnp.zeros_like(row))
        return 0

    lax.fori_loop(0, 48, pick, 0)
    lane48 = iota((48, 128), 1)
    for b in range(4):
        sides = []
        for e in range(2):
            halves = []
            for h in range(2):
                acc = jnp.zeros((48, 128), F32)
                for c in range(8):
                    x = picked[pl.ds(8 * h + c, 48, stride=16), :]
                    moved = pltpu.roll(x, (16 * c - (32 * b + 16 * e)) % 128, 1)
                    acc = jnp.where((lane48 >= 16 * c) & (lane48 < 16 * c + 16), moved, acc)
                halves.append(acc.astype(BF))
            sides.append(jnp.concatenate(halves, axis=1))
        before, last = sides
        carry[b, 0] = jnp.dot(last, filt[1], preferred_element_type=F32)
        carry[b, 1] = jnp.dot(last, filt[2], preferred_element_type=F32)
        carry[b, 2] = jnp.dot(before, filt[2], preferred_element_type=F32)
    save_carry = pltpu.make_async_copy(carry.at[3], carry_out_ref, out_sem.at[3])
    save_carry.start()

    pending = None
    for b in range(EARLY):
        if b == 2:
            arrived(2)
        if pending is not None:
            pending.wait()

        def make(i, _):
            gs = [3 * i + u for u in range(3)]
            bands = [band(recv[b], order_ref, live, g, slots if b == 1 else 0) for g in gs]
            for g, y in zip(gs, synthesise(bands, gs, carry.at[b], filt, one, two, mix)):
                stage[g] = y
            return 0

        lax.fori_loop(0, 16, make, 0)
        pending = pltpu.make_async_copy(stage, early_ref.at[b], out_sem.at[1])
        pending.start()
    arrived(3)
    save_last = pltpu.make_async_copy(recv[3], last_ref, out_sem.at[2])
    save_last.start()

    def drain(k, _):
        for b in (2, 3):
            far, near, apart = pair(b, k, 0, width[b])
            far.wait_send()

            @pl.when(apart)
            def _():
                near.wait_send()
        return 0

    lax.fori_loop(0, 32, drain, 0)
    pending.wait()
    save_filter.wait()
    save_last.wait()
    save_carry.wait()


def finish_kernel(
    order_ref, live_ref, early_ref, last_ref, filt_ref, carry_ref, out_ref,
    last, filt, carry, early, stage, one, two, mix, small_sem, in_sem, out_sem, stage_sem,
):
    small = [
        pltpu.make_async_copy(last_ref, last, small_sem.at[0]),
        pltpu.make_async_copy(filt_ref, filt, small_sem.at[1]),
        pltpu.make_async_copy(carry_ref, carry, small_sem.at[2]),
    ]
    for copy in small:
        copy.start()
    count = early.shape[0] // 12

    def take(i):
        return pltpu.make_async_copy(early_ref.at[pl.ds(count * i, count)], early.at[pl.ds(count * i, count)], in_sem.at[i])

    def give(i):
        return pltpu.make_async_copy(early.at[pl.ds(count * i, count)], out_ref.at[pl.ds(count * i, count)], out_sem.at[i])

    def put(i):
        return pltpu.make_async_copy(
            stage.at[pl.ds(4 * i, 4)], out_ref.at[pl.ds(48 * EARLY + 4 * i, 4)], stage_sem.at[i]
        )

    for i in range(12):
        take(i).start()
    for copy in small:
        copy.wait()
    live = live_ref[0]

    def make(i, _):
        gs = [4 * i + u for u in range(4)]
        bands = [band(last, order_ref, live, g) for g in gs]
        for g, y in zip(gs, synthesise(bands, gs, carry, filt, one, two, mix)):
            stage[g] = y
        take(i).wait()
        give(i).start()
        put(i).start()
        return 0

    lax.fori_loop(0, 12, make, 0)

    def close(i, _):
        give(i).wait()
        put(i).wait()
        return 0

    lax.fori_loop(0, 12, close, 0)


def on_device(sizes, voltages, pointing_table, beam_pointing, subband_order, live_subbands, filter_taps):
    slots = voltages.shape[0]
    devices = sizes[0] * sizes[1] * sizes[2] * sizes[3]
    volt = voltages.reshape(slots, 192, 1024)
    table = jnp.swapaxes(pointing_table, 2, 3)
    beams = beam_pointing.reshape(1, 256)
    coef = jnp.asarray(coefficient_rows())
    smem = pl.BlockSpec(memory_space=pltpu.SMEM)
    vmem = pl.BlockSpec(memory_space=pltpu.VMEM)
    hbm = pl.BlockSpec(memory_space=pl.ANY)
    VM = pltpu.VMEM
    def synth_scratch(n):
        return [VM((n, 136, 256), F32), VM((n, 136, 256), F32), VM((n, 256, 128), F32)]

    early, last, filt, carry = pl.pallas_call(
        functools.partial(exchange_kernel, *sizes),
        name="exchange",
        out_shape=[
            jax.ShapeDtypeStruct((EARLY, 48, 256, 128), BF),
            jax.ShapeDtypeStruct((devices * slots, 16, 128), BF),
            jax.ShapeDtypeStruct((3, 256, 256), BF),
            jax.ShapeDtypeStruct((3, 48, 256), F32),
        ],
        in_specs=[smem, smem, hbm, vmem, vmem, vmem, vmem],
        out_specs=[hbm] * 4,
        scratch_shapes=[
            VM((slots, 192, 1024), BF),
            VM((1024, 1024), BF),
            VM((512, 768), BF),
            VM((192, 768), BF),
            VM((slots, 192, 1024), BF),
            VM((1024, 128), F32),
            VM((4, devices, slots + 1, 16, 128), BF),
            VM((devices * slots, 16, 128), BF),
            VM((devices * (slots + 1), 16, 128), BF),
            VM((devices * slots, 16, 128), BF),
            VM((devices * slots, 16, 128), BF),
            VM((3, 256, 256), BF),
            VM((512, 128), F32),
            VM((16 * devices, 128), F32),
            VM((slots, 16, 192), BF),
            VM((slots, 16, 192), BF),
            VM((768, 128), F32),
            VM((4, 3, 48, 256), F32),
            *synth_scratch(3),
            VM((48, 256, 128), BF),
            pltpu.SemaphoreType.DMA((2, 2, 32)),
            pltpu.SemaphoreType.DMA((4,)),
            pltpu.SemaphoreType.DMA((2,)),
            pltpu.SemaphoreType.DMA((4,)),
            pltpu.SemaphoreType.DMA((2,)),
        ],
        compiler_params=pltpu.CompilerParams(
            collective_id=0, has_side_effects=True, vmem_limit_bytes=62 * 1024 * 1024
        ),
    )(subband_order, live_subbands, volt, table, beams, filter_taps, coef)

    out = pl.pallas_call(
        finish_kernel,
        name="finish",
        out_shape=jax.ShapeDtypeStruct((192, 256, 128), BF),
        in_specs=[smem, smem, hbm, hbm, hbm, hbm],
        out_specs=hbm,
        scratch_shapes=[
            VM((devices * slots, 16, 128), BF),
            VM((3, 256, 256), BF),
            VM((3, 48, 256), F32),
            VM((48 * EARLY, 256, 128), BF),
            VM((48, 256, 128), BF),
            *synth_scratch(4),
            pltpu.SemaphoreType.DMA((3,)),
            pltpu.SemaphoreType.DMA((12,)),
            pltpu.SemaphoreType.DMA((12,)),
            pltpu.SemaphoreType.DMA((12,)),
        ],
        compiler_params=pltpu.CompilerParams(vmem_limit_bytes=60 * 1024 * 1024),
    )(subband_order, live_subbands, early.reshape(48 * EARLY, 256, 128), last, filt, carry)
    out = out.reshape(4, 48, 128, 2, 128)
    return jnp.swapaxes(out, 2, 3).reshape(4, 48, 2, 16384)


def solution(mesh):
    sizes = (2, 4, 4, 2)
    in_specs = (P("sub", None, None, "tm"), P("sub", None, None, None), P(), P(), P(), P())
    out_specs = P("sub", None, None, "tm")
    return jax.shard_map(
        functools.partial(on_device, sizes), mesh=mesh, in_specs=in_specs, out_specs=out_specs, check_vma=False
    )
```

```python
import functools

import jax
import jax.numpy as jnp
import numpy as np
from jax import lax
from jax.experimental import pallas as pl
from jax.experimental.pallas import tpu as pltpu
from jax.sharding import PartitionSpec as P

MESH = pl.DeviceIdType.MESH
BF = jnp.bfloat16
F32 = jnp.float32
NT = (((1,), (1,)), ((), ()))
EARLY = 3


def turns():
    phase = np.arange(16, dtype=np.float32) * np.float32(2.0 * np.pi / 16)
    return [
        [float(x) for x in f(phase).astype(np.float32).astype(jnp.bfloat16).astype(np.float32)]
        for f in (np.cos, np.sin)
    ]


def iota(shape, dim):
    return lax.broadcasted_iota(jnp.int32, shape, dim)


def build_filter(taps_ref, coef_ref, filt_ref):
    repeat = (iota((16, 128), 1) % 16 == iota((16, 128), 0)).astype(F32)
    taps = jnp.dot(taps_ref[...], repeat, precision=lax.Precision.HIGHEST, preferred_element_type=F32)
    lag = iota((8, 128), 1) // 16 - iota((8, 128), 0)
    row = iota((64, 128), 0)
    turn = (row % 16) * (iota((64, 128), 1) % 16) % 16
    cosine = jnp.zeros((64, 128), F32)
    sine = jnp.zeros((64, 128), F32)
    for m, (x, y) in enumerate(zip(*turns())):
        cosine = jnp.where(turn == m, x, cosine)
        sine = jnp.where(turn == m, y, sine)
    which = row // 16
    coef_ref[...] = jnp.where(which == 1, -sine, jnp.where(which == 2, sine, cosine))
    for d in range(3):
        tap = jnp.zeros((8, 128), F32)
        for j in range(16):
            tap = jnp.where(lag + 8 * d == j, jnp.broadcast_to(taps[j : j + 1], (8, 128)), tap)
        for q in range(2):
            for c in range(16):
                block = [
                    tap * coef_ref[(2 * q + p) * 16 + c : (2 * q + p) * 16 + c + 1, :] for p in range(2)
                ]
                filt_ref[d, 16 * c : 16 * c + 16, 128 * q : 128 * q + 128] = jnp.concatenate(
                    block, axis=0
                ).astype(BF)


def band(rows_ref, order_ref, live, group, gap=0):
    parts = []
    for c in range(16):
        f = group * 16 + c
        slot = order_ref[f]
        part = rows_ref[slot + slot // gap if gap else slot]
        parts.append(jnp.where(f < live, part, jnp.zeros_like(part)))
    return jnp.concatenate(parts, axis=0)


def synthesise(bands, groups, carry_ref, filt_ref, one_ref, two_ref, mix_ref):
    n = len(bands)
    zt = jnp.concatenate([z.T for z in bands], axis=0)
    now = jnp.dot(zt, filt_ref[0], preferred_element_type=F32)
    one = jnp.dot(zt, filt_ref[1], preferred_element_type=F32)
    two = jnp.dot(zt, filt_ref[2], preferred_element_type=F32)
    outs = []
    for i in range(n):
        one_ref[i, 8:136, :] = one[128 * i : 128 * i + 128]
        two_ref[i, 8:136, :] = two[128 * i : 128 * i + 128]
        one_ref[i, 7:8, :] = carry_ref[0, pl.ds(groups[i], 1), :]
        two_ref[i, 7:8, :] = carry_ref[1, pl.ds(groups[i], 1), :]
        two_ref[i, 6:7, :] = carry_ref[2, pl.ds(groups[i], 1), :]
        total = now[128 * i : 128 * i + 128] + one_ref[i, 7:135, :] + two_ref[i, 6:134, :]
        mix_ref[i, pl.ds(0, 128, stride=2), :] = total[:, :128]
        mix_ref[i, pl.ds(1, 128, stride=2), :] = total[:, 128:]
        outs.append(mix_ref[i].astype(BF))
    return outs


def exchange_kernel(
    x_parts, z_parts, y_parts, c_parts,
    order_hbm, live_ref, volt_ref, table_hbm, beam_hbm, taps_hbm,
    early0, early1, early2, last_ref, filt_out_ref, carry_out_ref,
    order_ref, table_ref, beam_ref, taps_ref, coef_ref, volt, perm, hot, stack, rows, send, recv0, recv1, recv2, filt, ends, edge, tail_send, tail_recv, picked, carry,
    one, two, mix,
    send_sem, recv_sem, edge_sem, out_sem, load_sem, table_sem,
):
    recv = (recv0, recv1, recv2, last_ref)
    early = (early0, early1, early2)
    me = lax.axis_index("sub")
    half = lax.axis_index("tm")
    devices = x_parts * z_parts * y_parts * c_parts
    slots = volt_ref.shape[0]
    live = live_ref[0]
    width = (slots, slots + 1, slots, slots)

    barrier = pltpu.get_barrier_semaphore()

    tail_recv[...] = jnp.zeros_like(tail_recv)
    ends[...] = jnp.zeros_like(ends)

    def greet(i, _):
        @pl.when(i != me)
        def _():
            pl.semaphore_signal(barrier, inc=1, device_id=(i, half), device_id_type=MESH)

        return 0

    lax.fori_loop(0, devices, greet, 0)
    pl.semaphore_signal(barrier, inc=1, device_id=(me, 1 - half), device_id_type=MESH)

    load = [
        pltpu.make_async_copy(volt_ref.at[pl.ds(6 * h, 6)], volt.at[pl.ds(6 * h, 6)], load_sem.at[h])
        for h in range(2)
    ]
    tables = [
        pltpu.make_async_copy(beam_hbm, beam_ref, table_sem.at[0]),
        pltpu.make_async_copy(table_hbm, table_ref, table_sem.at[1]),
        pltpu.make_async_copy(taps_hbm, taps_ref, table_sem.at[2]),
        pltpu.make_async_copy(order_hbm, order_ref, table_sem.at[3]),
    ]
    tables[0].start()
    load[0].start()
    tables[1].start()
    load[1].start()
    for copy in tables[2:]:
        copy.start()
    def fill(i, _):
        ahead = iota((128, 128), 0) + 128 * i - 8 * iota((128, 128), 1)
        for t in range(8):
            perm[pl.ds(pl.multiple_of(128 * i, 128), 128), 128 * t : 128 * t + 128] = (ahead == t).astype(F32).astype(BF)
        return 0

    lax.fori_loop(0, 8, fill, 0)
    tables[0].wait()
    for b in range(4):
        row = iota((128, 256), 0)
        pick = iota((128, 256), 1) == 4 * (row // 2) + b
        key = jnp.sum(
            jnp.where(pick, jnp.broadcast_to(beam_ref[...].astype(F32), (128, 256)), 0.0), axis=1, keepdims=True
        )
        key = key.astype(jnp.int32) + 384 * (iota((128, 1), 0) % 2)
        hot[128 * b : 128 * b + 128, :] = (iota((128, 768), 1) == key).astype(F32).astype(BF)
    for copy in tables[1:]:
        copy.wait()
    stack[...] = jnp.zeros_like(stack)
    part = slots // 2

    def peer(dx, dz, dy, dc):
        c = me % c_parts
        y = (me // c_parts) % y_parts
        z = (me // (c_parts * y_parts)) % z_parts
        x = me // (c_parts * y_parts * z_parts)
        return (
            ((x + dx) % x_parts * z_parts + (z + dz) % z_parts) * y_parts + (y + dy) % y_parts
        ) * c_parts + (c + dc) % c_parts

    def pair(b, j, lo, count):
        dy = j % y_parts
        dz = (j // y_parts) % z_parts
        dc = j // (y_parts * z_parts)
        far = peer(1, dz, dy, dc)
        near = peer(0, dz + z_parts // 2, dy + y_parts // 2, dc)

        def copy(target, i):
            return pltpu.make_async_remote_copy(
                src_ref=send.at[b, target, pl.ds(lo, count)],
                dst_ref=recv[b].at[pl.ds(me * width[b] + lo, count)],
                send_sem=send_sem.at[i, b % 2, j],
                recv_sem=recv_sem.at[b],
                device_id=(target, half),
                device_id_type=MESH,
            )

        return copy(far, 0), copy(near, 1), near != me

    def ship(b, j, first, lo, count):
        far, near, apart = pair(b, j, lo, count)
        if not first:
            old_far, old_near, _ = pair(b - 2, j, 0, width[b - 2])
            old_far.wait_send()
        far.start()

        @pl.when(apart)
        def _():
            if not first:
                old_near.wait_send()
            near.start()

    def ship_range(b, lo, hi, first=False, slot=0, count=None):
        def step(j, _):
            ship(b, j, first, slot, width[b] if count is None else count)
            return 0

        lax.fori_loop(lo, hi, step, 0)

    def sort(s, _):
        parts = [
            jnp.dot(volt[s], perm[:, 256 * n : 256 * n + 256], preferred_element_type=F32).astype(BF)
            for n in range(4)
        ]
        for n in range(4):
            volt[s, :, 256 * n : 256 * n + 256] = parts[n]
        return 0

    def weights(s, lo, hi):
        real, imag = table_ref[s, 0], table_ref[s, 1]
        stack[0:96, 0:320] = real
        stack[0:96, 384:704] = imag
        stack[96:192, 0:320] = -imag
        stack[96:192, 384:704] = real
        return lax.dot_general(hot[lo:hi, :], stack[...], NT, preferred_element_type=F32).astype(BF)

    def form_slot(b, s):
        weight = weights(s, 128 * b, 128 * b + 128)
        for n in range(4):
            out = jnp.dot(weight, volt[s, :, 256 * n : 256 * n + 256], preferred_element_type=F32)
            rows[pl.ds(2 * n, 128, stride=8), :] = out[:, :128]
            rows[pl.ds(2 * n + 1, 128, stride=8), :] = out[:, 128:]
        send[b, :, s] = rows[...].astype(BF).reshape(devices, 16, 128)

    def keep_own(b, lo, hi):
        recv[b][pl.ds(me * width[b] + lo, hi - lo)] = send[b, me, lo:hi]

    def form_beam(b):
        def form(s, _):
            form_slot(b, s)
            return 0

        lax.fori_loop(0, slots, form, 0)
        keep_own(b, 0, width[b])

    def begin(s, _):
        sort(s, 0)
        form_slot(0, s)
        return 0

    hand_on = pltpu.make_async_remote_copy(
        src_ref=tail_send,
        dst_ref=tail_recv,
        send_sem=edge_sem.at[0],
        recv_sem=edge_sem.at[1],
        device_id=(me, 1),
        device_id_type=MESH,
    )

    quarter = part // 2
    for copy in load:
        copy.wait()
    pick_tail = (iota((16, 128), 1) == iota((16, 128), 0) + 112).astype(F32).astype(BF)
    for s in range(slots):
        tail_send[s] = lax.dot_general(pick_tail, volt[s, :, 896:1024], NT, preferred_element_type=F32).astype(BF)
    for lo, count, h in ((0, quarter, 0), (quarter, part - quarter, 0), (part, part, 1)):
        lax.fori_loop(lo, lo + count, begin, 0)
        keep_own(0, lo, lo + count)
        if lo == 0:
            pl.semaphore_wait(barrier, devices)
            @pl.when(half == 0)
            def _():
                hand_on.start()
        ship_range(0, 0, 32, True, lo, count)
    lane = iota((devices, 128), 1)

    def tails(s, _):
        ends[:, 0:16] = lax.dot_general(weights(s, 0, 512), tail_recv[s], NT, preferred_element_type=F32)
        total = jnp.zeros((devices, 128), F32)
        for b in range(4):
            for p in range(2):
                x = ends[pl.ds(128 * b + p, devices, stride=2), :]
                for e in range(2):
                    to = 32 * b + 16 * e + 8 * p
                    moved = pltpu.roll(x, (to - 8 * e) % 128, 1)
                    total = jnp.where((lane >= to) & (lane < to + 8), moved, total)
        edge[pl.ds(s, devices, stride=16), :] = total
        return 0

    @pl.when(half == 0)
    def _():
        hand_on.wait_send()

    @pl.when(half == 1)
    def _():
        hand_on.wait_recv()

    edge[...] = jnp.zeros_like(edge)
    lax.fori_loop(0, slots, tails, 0)
    send[1, :, slots] = edge[...].astype(BF).reshape(devices, 16, 128)
    form_beam(1)
    ship_range(1, 0, 32, True)
    form_beam(2)
    form_beam(3)
    ship_range(2, 0, 32)
    ship_range(3, 0, 32)
    build_filter(taps_ref, coef_ref, filt)
    save_filter = pltpu.make_async_copy(filt, filt_out_ref, out_sem.at[0])
    save_filter.start()

    def arrived(b):
        blocks = (devices - 1) * width[b]
        pltpu.make_async_remote_copy(
            src_ref=recv[b].at[pl.ds(0, blocks)],
            dst_ref=recv[b].at[pl.ds(0, blocks)],
            send_sem=send_sem.at[0, 0],
            recv_sem=recv_sem.at[b],
            device_id=(me, 1 - half),
            device_id_type=MESH,
        ).wait_recv()

    arrived(0)
    arrived(1)
    def unpack(d, _):
        edge[pl.ds(pl.multiple_of(16 * d, 16), 16), :] = recv[1][width[1] * d + slots].astype(F32)
        return 0

    lax.fori_loop(0, devices, unpack, 0)

    def pick(g, _):
        for c in range(16):
            f = 16 * g + c
            slot = order_ref[f]
            row = edge[pl.ds(slot + 4 * (slot // slots), 1), :]
            picked[pl.ds(f, 1), :] = jnp.where(f < live, row, jnp.zeros_like(row))
        return 0

    lax.fori_loop(0, 48, pick, 0)
    lane48 = iota((48, 128), 1)
    for b in range(4):
        sides = []
        for e in range(2):
            halves = []
            for h in range(2):
                acc = jnp.zeros((48, 128), F32)
                for c in range(8):
                    x = picked[pl.ds(8 * h + c, 48, stride=16), :]
                    moved = pltpu.roll(x, (16 * c - (32 * b + 16 * e)) % 128, 1)
                    acc = jnp.where((lane48 >= 16 * c) & (lane48 < 16 * c + 16), moved, acc)
                halves.append(acc.astype(BF))
            sides.append(jnp.concatenate(halves, axis=1))
        before, last = sides
        carry[b, 0] = jnp.dot(last, filt[1], preferred_element_type=F32)
        carry[b, 1] = jnp.dot(last, filt[2], preferred_element_type=F32)
        carry[b, 2] = jnp.dot(before, filt[2], preferred_element_type=F32)
    save_carry = pltpu.make_async_copy(carry.at[3], carry_out_ref, out_sem.at[3])
    save_carry.start()

    for b in range(EARLY):
        if b == 2:
            arrived(2)

        def make(i, _):
            gs = [3 * i + u for u in range(3)]
            bands = [band(recv[b], order_ref, live, g, slots if b == 1 else 0) for g in gs]
            for g, y in zip(gs, synthesise(bands, gs, carry.at[b], filt, one, two, mix)):
                early[b][g] = y
            return 0

        lax.fori_loop(0, 16, make, 0)
    arrived(3)

    def drain(k, _):
        for b in (2, 3):
            far, near, apart = pair(b, k, 0, width[b])
            far.wait_send()

            @pl.when(apart)
            def _():
                near.wait_send()
        return 0

    lax.fori_loop(0, 32, drain, 0)
    save_filter.wait()
    save_carry.wait()


def finish_kernel(
    order_hbm, live_ref, early0, early1, early2, last_ref, filt_ref, carry_ref, out_ref,
    order_ref, filt, carry, stage, one, two, mix, small_sem, out_sem, stage_sem,
):
    small = [
        pltpu.make_async_copy(filt_ref, filt, small_sem.at[0]),
        pltpu.make_async_copy(carry_ref, carry, small_sem.at[1]),
        pltpu.make_async_copy(order_hbm, order_ref, small_sem.at[2]),
    ]
    give = [
        pltpu.make_async_copy(ref, out_ref.at[pl.ds(48 * b, 48)], out_sem.at[b])
        for b, ref in enumerate((early0, early1, early2))
    ]
    for copy in small + give:
        copy.start()

    def put(i):
        return pltpu.make_async_copy(
            stage.at[pl.ds(4 * i, 4)], out_ref.at[pl.ds(48 * EARLY + 4 * i, 4)], stage_sem.at[i]
        )

    for copy in small:
        copy.wait()
    live = live_ref[0]

    def make(i, _):
        gs = [4 * i + u for u in range(4)]
        bands = [band(last_ref, order_ref, live, g) for g in gs]
        for g, y in zip(gs, synthesise(bands, gs, carry, filt, one, two, mix)):
            stage[g] = y
        put(i).start()
        return 0

    lax.fori_loop(0, 12, make, 0)

    def close(i, _):
        put(i).wait()
        return 0

    lax.fori_loop(0, 12, close, 0)
    for copy in give:
        copy.wait()


def on_device(sizes, voltages, pointing_table, beam_pointing, subband_order, live_subbands, filter_taps):
    slots = voltages.shape[0]
    devices = sizes[0] * sizes[1] * sizes[2] * sizes[3]
    volt = voltages.reshape(slots, 192, 1024)
    table = jnp.swapaxes(pointing_table, 2, 3)
    beams = beam_pointing.reshape(1, 256)
    smem = pl.BlockSpec(memory_space=pltpu.SMEM)
    vmem = pl.BlockSpec(memory_space=pltpu.VMEM)
    hbm = pl.BlockSpec(memory_space=pltpu.HBM)
    VM = pltpu.VMEM
    def synth_scratch(n):
        return [VM((n, 136, 256), F32), VM((n, 136, 256), F32), VM((n, 256, 128), F32)]

    early0, early1, early2, last, filt, carry = pl.pallas_call(
        functools.partial(exchange_kernel, *sizes),
        name="exchange",
        out_shape=[
            *[jax.ShapeDtypeStruct((48, 256, 128), BF)] * EARLY,
            jax.ShapeDtypeStruct((devices * slots, 16, 128), BF),
            jax.ShapeDtypeStruct((3, 256, 256), BF),
            jax.ShapeDtypeStruct((3, 48, 256), F32),
        ],
        in_specs=[hbm, smem, hbm, hbm, hbm, hbm],
        out_specs=[vmem] * 4 + [hbm] * 2,
        scratch_shapes=[
            pltpu.SMEM((768,), jnp.int32),
            VM((slots, 2, 96, 320), BF),
            VM((1, 256), jnp.int32),
            VM((16, 16), F32),
            VM((64, 128), F32),
            VM((slots, 192, 1024), BF),
            VM((1024, 1024), BF),
            VM((512, 768), BF),
            VM((192, 768), BF),
            VM((1024, 128), F32),
            VM((4, devices, slots + 1, 16, 128), BF),
            VM((devices * slots, 16, 128), BF),
            VM((devices * (slots + 1), 16, 128), BF),
            VM((devices * slots, 16, 128), BF),
            VM((3, 256, 256), BF),
            VM((512, 128), F32),
            VM((16 * devices, 128), F32),
            VM((slots, 16, 192), BF),
            VM((slots, 16, 192), BF),
            VM((768, 128), F32),
            VM((4, 3, 48, 256), F32),
            *synth_scratch(3),
            pltpu.SemaphoreType.DMA((2, 2, 32)),
            pltpu.SemaphoreType.DMA((4,)),
            pltpu.SemaphoreType.DMA((2,)),
            pltpu.SemaphoreType.DMA((4,)),
            pltpu.SemaphoreType.DMA((2,)),
            pltpu.SemaphoreType.DMA((4,)),
        ],
        compiler_params=pltpu.CompilerParams(
            collective_id=0, has_side_effects=True, vmem_limit_bytes=39 * 1024 * 1024
        ),
    )(subband_order, live_subbands, volt, table, beams, filter_taps)

    out = pl.pallas_call(
        finish_kernel,
        name="finish",
        out_shape=jax.ShapeDtypeStruct((192, 256, 128), BF),
        in_specs=[hbm, smem, vmem, vmem, vmem, vmem, hbm, hbm],
        out_specs=hbm,
        scratch_shapes=[
            pltpu.SMEM((768,), jnp.int32),
            VM((3, 256, 256), BF),
            VM((3, 48, 256), F32),
            VM((48, 256, 128), BF),
            *synth_scratch(4),
            pltpu.SemaphoreType.DMA((3,)),
            pltpu.SemaphoreType.DMA((3,)),
            pltpu.SemaphoreType.DMA((12,)),
        ],
        compiler_params=pltpu.CompilerParams(vmem_limit_bytes=12 * 1024 * 1024),
    )(subband_order, live_subbands, early0, early1, early2, last, filt, carry)
    out = out.reshape(4, 48, 128, 2, 128)
    return jnp.swapaxes(out, 2, 3).reshape(4, 48, 2, 16384)


def solution(mesh):
    sizes = (2, 4, 4, 2)
    in_specs = (P("sub", None, None, "tm"), P("sub", None, None, None), P(), P(), P(), P())
    out_specs = P("sub", None, None, "tm")
    return jax.shard_map(
        functools.partial(on_device, sizes), mesh=mesh, in_specs=in_specs, out_specs=out_specs, check_vma=False
    )
```

```python
import functools

import jax
import jax.numpy as jnp
import numpy as np
from jax import lax
from jax.experimental import pallas as pl
from jax.experimental.pallas import tpu as pltpu
from jax.sharding import PartitionSpec as P

MESH = pl.DeviceIdType.MESH
BF = jnp.bfloat16
F32 = jnp.float32
NT = (((1,), (1,)), ((), ()))
EARLY = 3


def turns():
    phase = np.arange(16, dtype=np.float32) * np.float32(2.0 * np.pi / 16)
    return [
        [float(x) for x in f(phase).astype(np.float32).astype(jnp.bfloat16).astype(np.float32)]
        for f in (np.cos, np.sin)
    ]


def iota(shape, dim):
    return lax.broadcasted_iota(jnp.int32, shape, dim)


def build_filter(taps_ref, coef_ref, filt_ref):
    repeat = (iota((16, 128), 1) % 16 == iota((16, 128), 0)).astype(F32)
    taps = jnp.dot(taps_ref[...], repeat, precision=lax.Precision.HIGHEST, preferred_element_type=F32)
    lag = iota((8, 128), 1) // 16 - iota((8, 128), 0)
    row = iota((64, 128), 0)
    turn = (row % 16) * (iota((64, 128), 1) % 16) % 16
    cosine = jnp.zeros((64, 128), F32)
    sine = jnp.zeros((64, 128), F32)
    for m, (x, y) in enumerate(zip(*turns())):
        cosine = jnp.where(turn == m, x, cosine)
        sine = jnp.where(turn == m, y, sine)
    which = row // 16
    coef_ref[...] = jnp.where(which == 1, -sine, jnp.where(which == 2, sine, cosine))
    for d in range(3):
        tap = jnp.zeros((8, 128), F32)
        for j in range(16):
            tap = jnp.where(lag + 8 * d == j, jnp.broadcast_to(taps[j : j + 1], (8, 128)), tap)
        for q in range(2):
            for c in range(16):
                block = [
                    tap * coef_ref[(2 * q + p) * 16 + c : (2 * q + p) * 16 + c + 1, :] for p in range(2)
                ]
                filt_ref[d, 16 * c : 16 * c + 16, 128 * q : 128 * q + 128] = jnp.concatenate(
                    block, axis=0
                ).astype(BF)


def band(rows_ref, order_ref, live, group, gap=0):
    parts = []
    for c in range(16):
        f = group * 16 + c
        slot = order_ref[f]
        part = rows_ref[slot + slot // gap if gap else slot]
        parts.append(jnp.where(f < live, part, jnp.zeros_like(part)))
    return jnp.concatenate(parts, axis=0)


def synthesise(bands, groups, carry_ref, filt_ref, one_ref, two_ref, mix_ref):
    n = len(bands)
    zt = jnp.concatenate([z.T for z in bands], axis=0)
    now = jnp.dot(zt, filt_ref[0], preferred_element_type=F32)
    one = jnp.dot(zt, filt_ref[1], preferred_element_type=F32)
    two = jnp.dot(zt, filt_ref[2], preferred_element_type=F32)
    outs = []
    for i in range(n):
        one_ref[i, 8:136, :] = one[128 * i : 128 * i + 128]
        two_ref[i, 8:136, :] = two[128 * i : 128 * i + 128]
        one_ref[i, 7:8, :] = carry_ref[0, pl.ds(groups[i], 1), :]
        two_ref[i, 7:8, :] = carry_ref[1, pl.ds(groups[i], 1), :]
        two_ref[i, 6:7, :] = carry_ref[2, pl.ds(groups[i], 1), :]
        total = now[128 * i : 128 * i + 128] + one_ref[i, 7:135, :] + two_ref[i, 6:134, :]
        mix_ref[i, pl.ds(0, 128, stride=2), :] = total[:, :128]
        mix_ref[i, pl.ds(1, 128, stride=2), :] = total[:, 128:]
        outs.append(mix_ref[i].astype(BF))
    return outs


def exchange_kernel(
    x_parts, z_parts, y_parts, c_parts,
    order_hbm, live_ref, volt_ref, table_hbm, beam_hbm, taps_hbm,
    early0, early1, early2, last_ref, filt_out_ref, carry_out_ref,
    order_ref, table_ref, beam_ref, taps_ref, coef_ref, volt, perm, hot, stack, rows, send, recv0, recv1, recv2, filt, ends, edge, tail_send, tail_recv, picked, carry,
    one, two, mix,
    send_sem, recv_sem, edge_sem, out_sem, load_sem, table_sem,
):
    recv = (recv0, recv1, recv2, last_ref)
    early = (early0, early1, early2)
    me = lax.axis_index("sub")
    half = lax.axis_index("tm")
    devices = x_parts * z_parts * y_parts * c_parts
    slots = volt_ref.shape[0]
    live = live_ref[0]
    width = (slots, slots + 1, slots, slots)

    barrier = pltpu.get_barrier_semaphore()

    tail_recv[...] = jnp.zeros_like(tail_recv)
    ends[...] = jnp.zeros_like(ends)

    def greet(i, _):
        @pl.when(i != me)
        def _():
            pl.semaphore_signal(barrier, inc=1, device_id=(i, half), device_id_type=MESH)

        return 0

    lax.fori_loop(0, devices, greet, 0)
    pl.semaphore_signal(barrier, inc=1, device_id=(me, 1 - half), device_id_type=MESH)

    load = [
        pltpu.make_async_copy(volt_ref.at[pl.ds(6 * h, 6)], volt.at[pl.ds(6 * h, 6)], load_sem.at[h])
        for h in range(2)
    ]
    tables = [
        pltpu.make_async_copy(beam_hbm, beam_ref, table_sem.at[0]),
        pltpu.make_async_copy(table_hbm, table_ref, table_sem.at[1]),
        pltpu.make_async_copy(taps_hbm, taps_ref, table_sem.at[2]),
        pltpu.make_async_copy(order_hbm, order_ref, table_sem.at[3]),
    ]
    tables[0].start()
    load[0].start()
    tables[1].start()
    load[1].start()
    for copy in tables[2:]:
        copy.start()
    def fill(i, _):
        ahead = iota((128, 128), 0) + 128 * i - 8 * iota((128, 128), 1)
        for t in range(8):
            perm[pl.ds(pl.multiple_of(128 * i, 128), 128), 128 * t : 128 * t + 128] = (ahead == t).astype(F32).astype(BF)
        return 0

    lax.fori_loop(0, 8, fill, 0)
    tables[0].wait()
    for b in range(4):
        row = iota((128, 256), 0)
        pick = iota((128, 256), 1) == 4 * (row // 2) + b
        key = jnp.sum(
            jnp.where(pick, jnp.broadcast_to(beam_ref[...].astype(F32), (128, 256)), 0.0), axis=1, keepdims=True
        )
        key = key.astype(jnp.int32) + 384 * (iota((128, 1), 0) % 2)
        hot[128 * b : 128 * b + 128, :] = (iota((128, 768), 1) == key).astype(F32).astype(BF)
    for copy in tables[1:]:
        copy.wait()
    stack[...] = jnp.zeros_like(stack)
    part = slots // 2

    def peer(dx, dz, dy, dc):
        c = me % c_parts
        y = (me // c_parts) % y_parts
        z = (me // (c_parts * y_parts)) % z_parts
        x = me // (c_parts * y_parts * z_parts)
        return (
            ((x + dx) % x_parts * z_parts + (z + dz) % z_parts) * y_parts + (y + dy) % y_parts
        ) * c_parts + (c + dc) % c_parts

    def pair(b, j, lo, count):
        dy = j % y_parts
        dz = (j // y_parts) % z_parts
        dc = j // (y_parts * z_parts)
        far = peer(1, dz, dy, dc)
        near = peer(0, dz + z_parts // 2, dy + y_parts // 2, dc)

        def copy(target, i):
            return pltpu.make_async_remote_copy(
                src_ref=send.at[b, target, pl.ds(lo, count)],
                dst_ref=recv[b].at[pl.ds(me * width[b] + lo, count)],
                send_sem=send_sem.at[i, b % 2, j],
                recv_sem=recv_sem.at[b],
                device_id=(target, half),
                device_id_type=MESH,
            )

        return copy(far, 0), copy(near, 1), near != me

    def ship(b, j, first, lo, count):
        far, near, apart = pair(b, j, lo, count)
        if not first:
            old_far, old_near, _ = pair(b - 2, j, 0, width[b - 2])
            old_far.wait_send()
        far.start()

        @pl.when(apart)
        def _():
            if not first:
                old_near.wait_send()
            near.start()

    def ship_range(b, lo, hi, first=False, slot=0, count=None):
        def step(j, _):
            ship(b, j, first, slot, width[b] if count is None else count)
            return 0

        lax.fori_loop(lo, hi, step, 0)

    def sort(s, _):
        parts = [
            jnp.dot(volt[s], perm[:, 256 * n : 256 * n + 256], preferred_element_type=F32).astype(BF)
            for n in range(4)
        ]
        for n in range(4):
            volt[s, :, 256 * n : 256 * n + 256] = parts[n]
        return 0

    def weights(s, lo, hi):
        real, imag = table_ref[s, 0], table_ref[s, 1]
        stack[0:96, 0:320] = real
        stack[0:96, 384:704] = imag
        stack[96:192, 0:320] = -imag
        stack[96:192, 384:704] = real
        return lax.dot_general(hot[lo:hi, :], stack[...], NT, preferred_element_type=F32).astype(BF)

    def form_slot(b, s):
        weight = weights(s, 128 * b, 128 * b + 128)
        for n in range(4):
            out = jnp.dot(weight, volt[s, :, 256 * n : 256 * n + 256], preferred_element_type=F32)
            rows[pl.ds(2 * n, 128, stride=8), :] = out[:, :128]
            rows[pl.ds(2 * n + 1, 128, stride=8), :] = out[:, 128:]
        send[b, :, s] = rows[...].astype(BF).reshape(devices, 16, 128)

    def keep_own(b, lo, hi):
        recv[b][pl.ds(me * width[b] + lo, hi - lo)] = send[b, me, lo:hi]

    def form_beam(b):
        def form(s, _):
            form_slot(b, s)
            return 0

        lax.fori_loop(0, slots, form, 0)
        keep_own(b, 0, width[b])

    def begin(s, _):
        sort(s, 0)
        form_slot(0, s)
        return 0

    hand_on = pltpu.make_async_remote_copy(
        src_ref=tail_send,
        dst_ref=tail_recv,
        send_sem=edge_sem.at[0],
        recv_sem=edge_sem.at[1],
        device_id=(me, 1),
        device_id_type=MESH,
    )

    quarter = part // 2
    for copy in load:
        copy.wait()
    pick_tail = (iota((16, 128), 1) == iota((16, 128), 0) + 112).astype(F32).astype(BF)
    for s in range(slots):
        tail_send[s] = lax.dot_general(pick_tail, volt[s, :, 896:1024], NT, preferred_element_type=F32).astype(BF)
    for lo, count, h in ((0, quarter, 0), (quarter, part - quarter, 0), (part, part, 1)):
        lax.fori_loop(lo, lo + count, begin, 0)
        keep_own(0, lo, lo + count)
        if lo == 0:
            pl.semaphore_wait(barrier, devices)
            @pl.when(half == 0)
            def _():
                hand_on.start()
        ship_range(0, 0, 32, True, lo, count)
    lane = iota((devices, 128), 1)

    def tails(s, _):
        ends[:, 0:16] = lax.dot_general(weights(s, 0, 512), tail_recv[s], NT, preferred_element_type=F32)
        total = jnp.zeros((devices, 128), F32)
        for b in range(4):
            for p in range(2):
                x = ends[pl.ds(128 * b + p, devices, stride=2), :]
                for e in range(2):
                    to = 32 * b + 16 * e + 8 * p
                    moved = pltpu.roll(x, (to - 8 * e) % 128, 1)
                    total = jnp.where((lane >= to) & (lane < to + 8), moved, total)
        edge[pl.ds(s, devices, stride=16), :] = total
        return 0

    @pl.when(half == 0)
    def _():
        hand_on.wait_send()

    @pl.when(half == 1)
    def _():
        hand_on.wait_recv()

    edge[...] = jnp.zeros_like(edge)
    lax.fori_loop(0, slots, tails, 0)
    send[1, :, slots] = edge[...].astype(BF).reshape(devices, 16, 128)
    form_beam(1)
    ship_range(1, 0, 32, True)
    form_beam(2)
    form_beam(3)
    ship_range(2, 0, 32)
    ship_range(3, 0, 32)
    build_filter(taps_ref, coef_ref, filt)
    save_filter = pltpu.make_async_copy(filt, filt_out_ref, out_sem.at[0])
    save_filter.start()

    def arrived(b):
        blocks = (devices - 1) * width[b]
        pltpu.make_async_remote_copy(
            src_ref=recv[b].at[pl.ds(0, blocks)],
            dst_ref=recv[b].at[pl.ds(0, blocks)],
            send_sem=send_sem.at[0, 0],
            recv_sem=recv_sem.at[b],
            device_id=(me, 1 - half),
            device_id_type=MESH,
        ).wait_recv()

    arrived(0)
    arrived(1)
    def unpack(d, _):
        edge[pl.ds(pl.multiple_of(16 * d, 16), 16), :] = recv[1][width[1] * d + slots].astype(F32)
        return 0

    lax.fori_loop(0, devices, unpack, 0)

    def pick(g, _):
        for c in range(16):
            f = 16 * g + c
            slot = order_ref[f]
            row = edge[pl.ds(slot + 4 * (slot // slots), 1), :]
            picked[pl.ds(f, 1), :] = jnp.where(f < live, row, jnp.zeros_like(row))
        return 0

    lax.fori_loop(0, 48, pick, 0)
    lane48 = iota((48, 128), 1)
    for b in range(4):
        sides = []
        for e in range(2):
            halves = []
            for h in range(2):
                acc = jnp.zeros((48, 128), F32)
                for c in range(8):
                    x = picked[pl.ds(8 * h + c, 48, stride=16), :]
                    moved = pltpu.roll(x, (16 * c - (32 * b + 16 * e)) % 128, 1)
                    acc = jnp.where((lane48 >= 16 * c) & (lane48 < 16 * c + 16), moved, acc)
                halves.append(acc.astype(BF))
            sides.append(jnp.concatenate(halves, axis=1))
        before, last = sides
        carry[b, 0] = jnp.dot(last, filt[1], preferred_element_type=F32)
        carry[b, 1] = jnp.dot(last, filt[2], preferred_element_type=F32)
        carry[b, 2] = jnp.dot(before, filt[2], preferred_element_type=F32)
    save_carry = pltpu.make_async_copy(carry.at[3], carry_out_ref, out_sem.at[3])
    save_carry.start()

    for b in range(EARLY):
        if b == 2:
            arrived(2)

        def make(i, _):
            gs = [3 * i + u for u in range(3)]
            bands = [band(recv[b], order_ref, live, g, slots if b == 1 else 0) for g in gs]
            for g, y in zip(gs, synthesise(bands, gs, carry.at[b], filt, one, two, mix)):
                early[b][g] = y
            return 0

        lax.fori_loop(0, 16, make, 0)
    arrived(3)

    def drain(k, _):
        for b in (2, 3):
            far, near, apart = pair(b, k, 0, width[b])
            far.wait_send()

            @pl.when(apart)
            def _():
                near.wait_send()
        return 0

    lax.fori_loop(0, 32, drain, 0)
    save_filter.wait()
    save_carry.wait()


def finish_kernel(
    order_hbm, live_ref, early0, early1, early2, last_ref, filt_ref, carry_ref, out_ref,
    order_ref, filt, carry, stage, one, two, mix, small_sem, out_sem, stage_sem,
):
    small = [
        pltpu.make_async_copy(filt_ref, filt, small_sem.at[0]),
        pltpu.make_async_copy(carry_ref, carry, small_sem.at[1]),
        pltpu.make_async_copy(order_hbm, order_ref, small_sem.at[2]),
    ]
    give = [
        pltpu.make_async_copy(ref, out_ref.at[pl.ds(48 * b, 48)], out_sem.at[b])
        for b, ref in enumerate((early0, early1, early2))
    ]
    for copy in small + give:
        copy.start()

    def put(i):
        return pltpu.make_async_copy(
            stage.at[pl.ds(4 * i, 4)], out_ref.at[pl.ds(48 * EARLY + 4 * i, 4)], stage_sem.at[i]
        )

    for copy in small:
        copy.wait()
    live = live_ref[0]

    def make(i, _):
        gs = [4 * i + u for u in range(4)]
        bands = [band(last_ref, order_ref, live, g) for g in gs]
        for g, y in zip(gs, synthesise(bands, gs, carry, filt, one, two, mix)):
            stage[g] = y
        put(i).start()
        return 0

    lax.fori_loop(0, 12, make, 0)

    def close(i, _):
        put(i).wait()
        return 0

    lax.fori_loop(0, 12, close, 0)
    for copy in give:
        copy.wait()


def on_device(sizes, voltages, pointing_table, beam_pointing, subband_order, live_subbands, filter_taps):
    slots = voltages.shape[0]
    devices = sizes[0] * sizes[1] * sizes[2] * sizes[3]
    volt = voltages.reshape(slots, 192, 1024)
    table = jnp.swapaxes(pointing_table, 2, 3)
    beams = beam_pointing.reshape(1, 256)
    table, beams, filter_taps, subband_order = (
        pltpu.with_memory_space_constraint(a, pltpu.HBM) for a in (table, beams, filter_taps, subband_order)
    )
    smem = pl.BlockSpec(memory_space=pltpu.SMEM)
    vmem = pl.BlockSpec(memory_space=pltpu.VMEM)
    hbm = pl.BlockSpec(memory_space=pltpu.HBM)
    VM = pltpu.VMEM
    def synth_scratch(n):
        return [VM((n, 136, 256), F32), VM((n, 136, 256), F32), VM((n, 256, 128), F32)]

    early0, early1, early2, last, filt, carry = pl.pallas_call(
        functools.partial(exchange_kernel, *sizes),
        name="exchange",
        out_shape=[
            *[jax.ShapeDtypeStruct((48, 256, 128), BF)] * EARLY,
            jax.ShapeDtypeStruct((devices * slots, 16, 128), BF),
            jax.ShapeDtypeStruct((3, 256, 256), BF),
            jax.ShapeDtypeStruct((3, 48, 256), F32),
        ],
        in_specs=[hbm, smem, hbm, hbm, hbm, hbm],
        out_specs=[vmem] * 4 + [hbm] * 2,
        scratch_shapes=[
            pltpu.SMEM((768,), jnp.int32),
            VM((slots, 2, 96, 320), BF),
            VM((1, 256), jnp.int32),
            VM((16, 16), F32),
            VM((64, 128), F32),
            VM((slots, 192, 1024), BF),
            VM((1024, 1024), BF),
            VM((512, 768), BF),
            VM((192, 768), BF),
            VM((1024, 128), F32),
            VM((4, devices, slots + 1, 16, 128), BF),
            VM((devices * slots, 16, 128), BF),
            VM((devices * (slots + 1), 16, 128), BF),
            VM((devices * slots, 16, 128), BF),
            VM((3, 256, 256), BF),
            VM((512, 128), F32),
            VM((16 * devices, 128), F32),
            VM((slots, 16, 192), BF),
            VM((slots, 16, 192), BF),
            VM((768, 128), F32),
            VM((4, 3, 48, 256), F32),
            *synth_scratch(3),
            pltpu.SemaphoreType.DMA((2, 2, 32)),
            pltpu.SemaphoreType.DMA((4,)),
            pltpu.SemaphoreType.DMA((2,)),
            pltpu.SemaphoreType.DMA((4,)),
            pltpu.SemaphoreType.DMA((2,)),
            pltpu.SemaphoreType.DMA((4,)),
        ],
        compiler_params=pltpu.CompilerParams(
            collective_id=0, has_side_effects=True, vmem_limit_bytes=39 * 1024 * 1024
        ),
    )(subband_order, live_subbands, volt, table, beams, filter_taps)

    out = pl.pallas_call(
        finish_kernel,
        name="finish",
        out_shape=jax.ShapeDtypeStruct((192, 256, 128), BF),
        in_specs=[hbm, smem, vmem, vmem, vmem, vmem, hbm, hbm],
        out_specs=hbm,
        scratch_shapes=[
            pltpu.SMEM((768,), jnp.int32),
            VM((3, 256, 256), BF),
            VM((3, 48, 256), F32),
            VM((48, 256, 128), BF),
            *synth_scratch(4),
            pltpu.SemaphoreType.DMA((3,)),
            pltpu.SemaphoreType.DMA((3,)),
            pltpu.SemaphoreType.DMA((12,)),
        ],
        compiler_params=pltpu.CompilerParams(vmem_limit_bytes=12 * 1024 * 1024),
    )(subband_order, live_subbands, early0, early1, early2, last, filt, carry)
    out = out.reshape(4, 48, 128, 2, 128)
    return jnp.swapaxes(out, 2, 3).reshape(4, 48, 2, 16384)


def solution(mesh):
    sizes = (2, 4, 4, 2)
    in_specs = (P("sub", None, None, "tm"), P("sub", None, None, None), P(), P(), P(), P())
    out_specs = P("sub", None, None, "tm")
    return jax.shard_map(
        functools.partial(on_device, sizes), mesh=mesh, in_specs=in_specs, out_specs=out_specs, check_vma=False
    )
```

```python
import functools

import jax
import jax.numpy as jnp
import numpy as np
from jax import lax
from jax.experimental import pallas as pl
from jax.experimental.pallas import tpu as pltpu
from jax.sharding import PartitionSpec as P

MESH = pl.DeviceIdType.MESH
BF = jnp.bfloat16
F32 = jnp.float32
NT = (((1,), (1,)), ((), ()))
EARLY = 3


def turns():
    phase = np.arange(16, dtype=np.float32) * np.float32(2.0 * np.pi / 16)
    return [
        [float(x) for x in f(phase).astype(np.float32).astype(jnp.bfloat16).astype(np.float32)]
        for f in (np.cos, np.sin)
    ]


def iota(shape, dim):
    return lax.broadcasted_iota(jnp.int32, shape, dim)


def build_filter(taps_ref, coef_ref, filt_ref):
    repeat = (iota((16, 128), 1) % 16 == iota((16, 128), 0)).astype(F32)
    taps = jnp.dot(taps_ref[...], repeat, precision=lax.Precision.HIGHEST, preferred_element_type=F32)
    lag = iota((8, 128), 1) // 16 - iota((8, 128), 0)
    row = iota((64, 128), 0)
    turn = (row % 16) * (iota((64, 128), 1) % 16) % 16
    cosine = jnp.zeros((64, 128), F32)
    sine = jnp.zeros((64, 128), F32)
    for m, (x, y) in enumerate(zip(*turns())):
        cosine = jnp.where(turn == m, x, cosine)
        sine = jnp.where(turn == m, y, sine)
    which = row // 16
    coef_ref[...] = jnp.where(which == 1, -sine, jnp.where(which == 2, sine, cosine))
    for d in range(3):
        tap = jnp.zeros((8, 128), F32)
        for j in range(16):
            tap = jnp.where(lag + 8 * d == j, jnp.broadcast_to(taps[j : j + 1], (8, 128)), tap)
        for q in range(2):
            for c in range(16):
                block = [
                    tap * coef_ref[(2 * q + p) * 16 + c : (2 * q + p) * 16 + c + 1, :] for p in range(2)
                ]
                filt_ref[d, 16 * c : 16 * c + 16, 128 * q : 128 * q + 128] = jnp.concatenate(
                    block, axis=0
                ).astype(BF)


def band(rows_ref, order_ref, live, group, gap=0):
    parts = []
    for c in range(16):
        f = group * 16 + c
        slot = order_ref[f]
        part = rows_ref[slot + slot // gap if gap else slot]
        parts.append(jnp.where(f < live, part, jnp.zeros_like(part)))
    return jnp.concatenate(parts, axis=0)


def synthesise(bands, groups, carry_ref, filt_ref, one_ref, two_ref, mix_ref):
    n = len(bands)
    zt = jnp.concatenate([z.T for z in bands], axis=0)
    now = jnp.dot(zt, filt_ref[0], preferred_element_type=F32)
    one = jnp.dot(zt, filt_ref[1], preferred_element_type=F32)
    two = jnp.dot(zt, filt_ref[2], preferred_element_type=F32)
    outs = []
    for i in range(n):
        one_ref[i, 8:136, :] = one[128 * i : 128 * i + 128]
        two_ref[i, 8:136, :] = two[128 * i : 128 * i + 128]
        one_ref[i, 7:8, :] = carry_ref[0, pl.ds(groups[i], 1), :]
        two_ref[i, 7:8, :] = carry_ref[1, pl.ds(groups[i], 1), :]
        two_ref[i, 6:7, :] = carry_ref[2, pl.ds(groups[i], 1), :]
        total = now[128 * i : 128 * i + 128] + one_ref[i, 7:135, :] + two_ref[i, 6:134, :]
        mix_ref[i, pl.ds(0, 128, stride=2), :] = total[:, :128]
        mix_ref[i, pl.ds(1, 128, stride=2), :] = total[:, 128:]
        outs.append(mix_ref[i].astype(BF))
    return outs


def exchange_kernel(
    x_parts, z_parts, y_parts, c_parts,
    order_hbm, live_ref, volt_ref, table_hbm, beam_hbm, taps_hbm,
    early0, early1, early2, last_ref, filt_out_ref, carry_out_ref,
    order_ref, table_ref, beam_ref, taps_ref, coef_ref, volt, perm, hot, stack, rows, send, recv0, recv1, recv2, filt, ends, edge, tail_send, tail_recv, picked, carry,
    one, two, mix,
    send_sem, recv_sem, edge_sem, out_sem, load_sem, table_sem,
):
    recv = (recv0, recv1, recv2, last_ref)
    early = (early0, early1, early2)
    me = lax.axis_index("sub")
    half = lax.axis_index("tm")
    devices = x_parts * z_parts * y_parts * c_parts
    slots = volt_ref.shape[0]
    live = live_ref[0]
    width = (slots, slots + 1, slots, slots)

    barrier = pltpu.get_barrier_semaphore()

    tail_recv[...] = jnp.zeros_like(tail_recv)
    ends[...] = jnp.zeros_like(ends)

    def greet(i, _):
        @pl.when(i != me)
        def _():
            pl.semaphore_signal(barrier, inc=1, device_id=(i, half), device_id_type=MESH)

        return 0

    lax.fori_loop(0, devices, greet, 0)
    pl.semaphore_signal(barrier, inc=1, device_id=(me, 1 - half), device_id_type=MESH)

    load = [
        pltpu.make_async_copy(volt_ref.at[pl.ds(6 * h, 6)], volt.at[pl.ds(6 * h, 6)], load_sem.at[h])
        for h in range(2)
    ]
    tables = [
        pltpu.make_async_copy(beam_hbm, beam_ref, table_sem.at[0]),
        pltpu.make_async_copy(table_hbm, table_ref, table_sem.at[1]),
        pltpu.make_async_copy(taps_hbm, taps_ref, table_sem.at[2]),
        pltpu.make_async_copy(order_hbm, order_ref, table_sem.at[3]),
    ]
    tables[0].start()
    load[0].start()
    tables[1].start()
    load[1].start()
    for copy in tables[2:]:
        copy.start()
    def fill(i, _):
        ahead = iota((128, 128), 0) + 128 * i - 8 * iota((128, 128), 1)
        for t in range(8):
            perm[pl.ds(pl.multiple_of(128 * i, 128), 128), 128 * t : 128 * t + 128] = (ahead == t).astype(F32).astype(BF)
        return 0

    lax.fori_loop(0, 8, fill, 0)
    tables[0].wait()
    for b in range(4):
        row = iota((128, 256), 0)
        pick = iota((128, 256), 1) == 4 * (row // 2) + b
        key = jnp.sum(
            jnp.where(pick, jnp.broadcast_to(beam_ref[...].astype(F32), (128, 256)), 0.0), axis=1, keepdims=True
        )
        key = key.astype(jnp.int32) + 384 * (iota((128, 1), 0) % 2)
        hot[128 * b : 128 * b + 128, :] = (iota((128, 768), 1) == key).astype(F32).astype(BF)
    for copy in tables[1:]:
        copy.wait()
    stack[...] = jnp.zeros_like(stack)
    part = slots // 2

    def peer(dx, dz, dy, dc):
        c = me % c_parts
        y = (me // c_parts) % y_parts
        z = (me // (c_parts * y_parts)) % z_parts
        x = me // (c_parts * y_parts * z_parts)
        return (
            ((x + dx) % x_parts * z_parts + (z + dz) % z_parts) * y_parts + (y + dy) % y_parts
        ) * c_parts + (c + dc) % c_parts

    def pair(b, j, lo, count):
        dy = j % y_parts
        dz = (j // y_parts) % z_parts
        dc = j // (y_parts * z_parts)
        far = peer(1, dz, dy, dc)
        near = peer(0, dz + z_parts // 2, dy + y_parts // 2, dc)

        def copy(target, i):
            return pltpu.make_async_remote_copy(
                src_ref=send.at[b, target, pl.ds(lo, count)],
                dst_ref=recv[b].at[pl.ds(me * width[b] + lo, count)],
                send_sem=send_sem.at[i, b % 2, j],
                recv_sem=recv_sem.at[b],
                device_id=(target, half),
                device_id_type=MESH,
            )

        return copy(far, 0), copy(near, 1), near != me

    def ship(b, j, first, lo, count):
        far, near, apart = pair(b, j, lo, count)
        if not first:
            old_far, old_near, _ = pair(b - 2, j, 0, width[b - 2])
            old_far.wait_send()
        far.start()

        @pl.when(apart)
        def _():
            if not first:
                old_near.wait_send()
            near.start()

    def ship_range(b, lo, hi, first=False, slot=0, count=None):
        def step(j, _):
            ship(b, j, first, slot, width[b] if count is None else count)
            return 0

        lax.fori_loop(lo, hi, step, 0)

    def sort(s, _):
        parts = [
            jnp.dot(volt[s], perm[:, 256 * n : 256 * n + 256], preferred_element_type=F32).astype(BF)
            for n in range(4)
        ]
        for n in range(4):
            volt[s, :, 256 * n : 256 * n + 256] = parts[n]
        return 0

    def weights(s, lo, hi):
        real, imag = table_ref[s, 0], table_ref[s, 1]
        stack[0:96, 0:320] = real
        stack[0:96, 384:704] = imag
        stack[96:192, 0:320] = -imag
        stack[96:192, 384:704] = real
        return lax.dot_general(hot[lo:hi, :], stack[...], NT, preferred_element_type=F32).astype(BF)

    def form_slot(b, s):
        weight = weights(s, 128 * b, 128 * b + 128)
        for n in range(4):
            out = jnp.dot(weight, volt[s, :, 256 * n : 256 * n + 256], preferred_element_type=F32)
            rows[pl.ds(2 * n, 128, stride=8), :] = out[:, :128]
            rows[pl.ds(2 * n + 1, 128, stride=8), :] = out[:, 128:]
        send[b, :, s] = rows[...].astype(BF).reshape(devices, 16, 128)

    def keep_own(b, lo, hi):
        recv[b][pl.ds(me * width[b] + lo, hi - lo)] = send[b, me, lo:hi]

    def form_beam(b):
        def form(s, _):
            form_slot(b, s)
            return 0

        lax.fori_loop(0, slots, form, 0)
        keep_own(b, 0, width[b])

    def begin(s, _):
        sort(s, 0)
        form_slot(0, s)
        return 0

    hand_on = pltpu.make_async_remote_copy(
        src_ref=tail_send,
        dst_ref=tail_recv,
        send_sem=edge_sem.at[0],
        recv_sem=edge_sem.at[1],
        device_id=(me, 1),
        device_id_type=MESH,
    )

    quarter = part // 2
    for copy in load:
        copy.wait()
    pick_tail = (iota((16, 128), 1) == iota((16, 128), 0) + 112).astype(F32).astype(BF)
    for s in range(slots):
        tail_send[s] = lax.dot_general(pick_tail, volt[s, :, 896:1024], NT, preferred_element_type=F32).astype(BF)
    for lo, count, h in ((0, quarter, 0), (quarter, part - quarter, 0), (part, part, 1)):
        lax.fori_loop(lo, lo + count, begin, 0)
        keep_own(0, lo, lo + count)
        if lo == 0:
            pl.semaphore_wait(barrier, devices)
            @pl.when(half == 0)
            def _():
                hand_on.start()
        ship_range(0, 0, 32, True, lo, count)
    lane = iota((devices, 128), 1)

    def tails(s, _):
        ends[:, 0:16] = lax.dot_general(weights(s, 0, 512), tail_recv[s], NT, preferred_element_type=F32)
        total = jnp.zeros((devices, 128), F32)
        for b in range(4):
            for p in range(2):
                x = ends[pl.ds(128 * b + p, devices, stride=2), :]
                for e in range(2):
                    to = 32 * b + 16 * e + 8 * p
                    moved = pltpu.roll(x, (to - 8 * e) % 128, 1)
                    total = jnp.where((lane >= to) & (lane < to + 8), moved, total)
        edge[pl.ds(s, devices, stride=16), :] = total
        return 0

    @pl.when(half == 0)
    def _():
        hand_on.wait_send()

    @pl.when(half == 1)
    def _():
        hand_on.wait_recv()

    edge[...] = jnp.zeros_like(edge)
    lax.fori_loop(0, slots, tails, 0)
    send[1, :, slots] = edge[...].astype(BF).reshape(devices, 16, 128)
    form_beam(1)
    ship_range(1, 0, 32, True)
    form_beam(2)
    form_beam(3)
    ship_range(2, 0, 32)
    ship_range(3, 0, 32)
    build_filter(taps_ref, coef_ref, filt)
    save_filter = pltpu.make_async_copy(filt, filt_out_ref, out_sem.at[0])
    save_filter.start()

    def arrived(b):
        blocks = (devices - 1) * width[b]
        pltpu.make_async_remote_copy(
            src_ref=recv[b].at[pl.ds(0, blocks)],
            dst_ref=recv[b].at[pl.ds(0, blocks)],
            send_sem=send_sem.at[0, 0],
            recv_sem=recv_sem.at[b],
            device_id=(me, 1 - half),
            device_id_type=MESH,
        ).wait_recv()

    arrived(0)
    arrived(1)
    def unpack(d, _):
        edge[pl.ds(pl.multiple_of(16 * d, 16), 16), :] = recv[1][width[1] * d + slots].astype(F32)
        return 0

    lax.fori_loop(0, devices, unpack, 0)

    def pick(g, _):
        for c in range(16):
            f = 16 * g + c
            slot = order_ref[f]
            row = edge[pl.ds(slot + 4 * (slot // slots), 1), :]
            picked[pl.ds(f, 1), :] = jnp.where(f < live, row, jnp.zeros_like(row))
        return 0

    lax.fori_loop(0, 48, pick, 0)
    lane48 = iota((48, 128), 1)
    for b in range(4):
        sides = []
        for e in range(2):
            halves = []
            for h in range(2):
                acc = jnp.zeros((48, 128), F32)
                for c in range(8):
                    x = picked[pl.ds(8 * h + c, 48, stride=16), :]
                    moved = pltpu.roll(x, (16 * c - (32 * b + 16 * e)) % 128, 1)
                    acc = jnp.where((lane48 >= 16 * c) & (lane48 < 16 * c + 16), moved, acc)
                halves.append(acc.astype(BF))
            sides.append(jnp.concatenate(halves, axis=1))
        before, last = sides
        carry[b, 0] = jnp.dot(last, filt[1], preferred_element_type=F32)
        carry[b, 1] = jnp.dot(last, filt[2], preferred_element_type=F32)
        carry[b, 2] = jnp.dot(before, filt[2], preferred_element_type=F32)
    save_carry = pltpu.make_async_copy(carry.at[3], carry_out_ref, out_sem.at[3])
    save_carry.start()

    for b in range(EARLY):
        if b == 2:
            arrived(2)

        def make(i, _):
            gs = [3 * i + u for u in range(3)]
            bands = [band(recv[b], order_ref, live, g, slots if b == 1 else 0) for g in gs]
            for g, y in zip(gs, synthesise(bands, gs, carry.at[b], filt, one, two, mix)):
                early[b][g] = y
            return 0

        lax.fori_loop(0, 16, make, 0)
    arrived(3)

    def drain(k, _):
        for b in (2, 3):
            far, near, apart = pair(b, k, 0, width[b])
            far.wait_send()

            @pl.when(apart)
            def _():
                near.wait_send()
        return 0

    lax.fori_loop(0, 32, drain, 0)
    save_filter.wait()
    save_carry.wait()


def finish_kernel(
    order_hbm, live_ref, early0, early1, early2, last_ref, filt_ref, carry_ref, out_ref,
    order_ref, filt, carry, stage, one, two, mix, small_sem, out_sem, stage_sem,
):
    small = [
        pltpu.make_async_copy(filt_ref, filt, small_sem.at[0]),
        pltpu.make_async_copy(carry_ref, carry, small_sem.at[1]),
        pltpu.make_async_copy(order_hbm, order_ref, small_sem.at[2]),
    ]
    give = [
        pltpu.make_async_copy(ref, out_ref.at[pl.ds(48 * b, 48)], out_sem.at[b])
        for b, ref in enumerate((early0, early1, early2))
    ]
    for copy in small + give:
        copy.start()

    def put(i):
        return pltpu.make_async_copy(
            stage.at[pl.ds(6 * i, 6)], out_ref.at[pl.ds(48 * EARLY + 6 * i, 6)], stage_sem.at[i]
        )

    for copy in small:
        copy.wait()
    live = live_ref[0]

    def make(i, _):
        gs = [6 * i + u for u in range(6)]
        bands = [band(last_ref, order_ref, live, g) for g in gs]
        for g, y in zip(gs, synthesise(bands, gs, carry, filt, one, two, mix)):
            stage[g] = y
        put(i).start()
        return 0

    lax.fori_loop(0, 8, make, 0)

    def close(i, _):
        put(i).wait()
        return 0

    lax.fori_loop(0, 8, close, 0)
    for copy in give:
        copy.wait()


def on_device(sizes, voltages, pointing_table, beam_pointing, subband_order, live_subbands, filter_taps):
    slots = voltages.shape[0]
    devices = sizes[0] * sizes[1] * sizes[2] * sizes[3]
    volt = voltages.reshape(slots, 192, 1024)
    table = jnp.swapaxes(pointing_table, 2, 3)
    beams = beam_pointing.reshape(1, 256)
    table, beams, filter_taps, subband_order = (
        pltpu.with_memory_space_constraint(a, pltpu.HBM) for a in (table, beams, filter_taps, subband_order)
    )
    smem = pl.BlockSpec(memory_space=pltpu.SMEM)
    vmem = pl.BlockSpec(memory_space=pltpu.VMEM)
    hbm = pl.BlockSpec(memory_space=pltpu.HBM)
    VM = pltpu.VMEM
    def synth_scratch(n):
        return [VM((n, 136, 256), F32), VM((n, 136, 256), F32), VM((n, 256, 128), F32)]

    early0, early1, early2, last, filt, carry = pl.pallas_call(
        functools.partial(exchange_kernel, *sizes),
        name="exchange",
        out_shape=[
            *[jax.ShapeDtypeStruct((48, 256, 128), BF)] * EARLY,
            jax.ShapeDtypeStruct((devices * slots, 16, 128), BF),
            jax.ShapeDtypeStruct((3, 256, 256), BF),
            jax.ShapeDtypeStruct((3, 48, 256), F32),
        ],
        in_specs=[hbm, smem, hbm, hbm, hbm, hbm],
        out_specs=[vmem] * 4 + [hbm] * 2,
        scratch_shapes=[
            pltpu.SMEM((768,), jnp.int32),
            VM((slots, 2, 96, 320), BF),
            VM((1, 256), jnp.int32),
            VM((16, 16), F32),
            VM((64, 128), F32),
            VM((slots, 192, 1024), BF),
            VM((1024, 1024), BF),
            VM((512, 768), BF),
            VM((192, 768), BF),
            VM((1024, 128), F32),
            VM((4, devices, slots + 1, 16, 128), BF),
            VM((devices * slots, 16, 128), BF),
            VM((devices * (slots + 1), 16, 128), BF),
            VM((devices * slots, 16, 128), BF),
            VM((3, 256, 256), BF),
            VM((512, 128), F32),
            VM((16 * devices, 128), F32),
            VM((slots, 16, 192), BF),
            VM((slots, 16, 192), BF),
            VM((768, 128), F32),
            VM((4, 3, 48, 256), F32),
            *synth_scratch(3),
            pltpu.SemaphoreType.DMA((2, 2, 32)),
            pltpu.SemaphoreType.DMA((4,)),
            pltpu.SemaphoreType.DMA((2,)),
            pltpu.SemaphoreType.DMA((4,)),
            pltpu.SemaphoreType.DMA((2,)),
            pltpu.SemaphoreType.DMA((4,)),
        ],
        compiler_params=pltpu.CompilerParams(
            collective_id=0, has_side_effects=True, vmem_limit_bytes=39 * 1024 * 1024
        ),
    )(subband_order, live_subbands, volt, table, beams, filter_taps)

    out = pl.pallas_call(
        finish_kernel,
        name="finish",
        out_shape=jax.ShapeDtypeStruct((192, 256, 128), BF),
        in_specs=[hbm, smem, vmem, vmem, vmem, vmem, hbm, hbm],
        out_specs=hbm,
        scratch_shapes=[
            pltpu.SMEM((768,), jnp.int32),
            VM((3, 256, 256), BF),
            VM((3, 48, 256), F32),
            VM((48, 256, 128), BF),
            *synth_scratch(6),
            pltpu.SemaphoreType.DMA((3,)),
            pltpu.SemaphoreType.DMA((3,)),
            pltpu.SemaphoreType.DMA((8,)),
        ],
        compiler_params=pltpu.CompilerParams(vmem_limit_bytes=12 * 1024 * 1024),
    )(subband_order, live_subbands, early0, early1, early2, last, filt, carry)
    out = out.reshape(4, 48, 128, 2, 128)
    return jnp.swapaxes(out, 2, 3).reshape(4, 48, 2, 16384)


def solution(mesh):
    sizes = (2, 4, 4, 2)
    in_specs = (P("sub", None, None, "tm"), P("sub", None, None, None), P(), P(), P(), P())
    out_specs = P("sub", None, None, "tm")
    return jax.shard_map(
        functools.partial(on_device, sizes), mesh=mesh, in_specs=in_specs, out_specs=out_specs, check_vma=False
    )
```

```python
import functools

import jax
import jax.numpy as jnp
import numpy as np
from jax import lax
from jax.experimental import pallas as pl
from jax.experimental.pallas import tpu as pltpu
from jax.sharding import PartitionSpec as P

MESH = pl.DeviceIdType.MESH
BF = jnp.bfloat16
F32 = jnp.float32
NT = (((1,), (1,)), ((), ()))
EARLY = 3


def turns():
    phase = np.arange(16, dtype=np.float32) * np.float32(2.0 * np.pi / 16)
    return [
        [float(x) for x in f(phase).astype(np.float32).astype(jnp.bfloat16).astype(np.float32)]
        for f in (np.cos, np.sin)
    ]


def iota(shape, dim):
    return lax.broadcasted_iota(jnp.int32, shape, dim)


def build_filter(taps_ref, coef_ref, filt_ref):
    repeat = (iota((16, 128), 1) % 16 == iota((16, 128), 0)).astype(F32)
    taps = jnp.dot(taps_ref[...], repeat, precision=lax.Precision.HIGHEST, preferred_element_type=F32)
    lag = iota((8, 128), 1) // 16 - iota((8, 128), 0)
    row = iota((64, 128), 0)
    turn = (row % 16) * (iota((64, 128), 1) % 16) % 16
    cosine = jnp.zeros((64, 128), F32)
    sine = jnp.zeros((64, 128), F32)
    for m, (x, y) in enumerate(zip(*turns())):
        cosine = jnp.where(turn == m, x, cosine)
        sine = jnp.where(turn == m, y, sine)
    which = row // 16
    coef_ref[...] = jnp.where(which == 1, -sine, jnp.where(which == 2, sine, cosine))
    for d in range(3):
        tap = jnp.zeros((8, 128), F32)
        for j in range(16):
            tap = jnp.where(lag + 8 * d == j, jnp.broadcast_to(taps[j : j + 1], (8, 128)), tap)
        for q in range(2):
            for c in range(16):
                block = [
                    tap * coef_ref[(2 * q + p) * 16 + c : (2 * q + p) * 16 + c + 1, :] for p in range(2)
                ]
                filt_ref[d, 16 * c : 16 * c + 16, 128 * q : 128 * q + 128] = jnp.concatenate(
                    block, axis=0
                ).astype(BF)


def band(rows_ref, order_ref, live, group, gap=0):
    parts = []
    for c in range(16):
        f = group * 16 + c
        slot = order_ref[f]
        part = rows_ref[slot + slot // gap if gap else slot]
        parts.append(jnp.where(f < live, part, jnp.zeros_like(part)))
    return jnp.concatenate(parts, axis=0)


def synthesise(bands, groups, carry_ref, filt_ref, one_ref, two_ref, mix_ref):
    n = len(bands)
    zt = jnp.concatenate([z.T for z in bands], axis=0)
    now = jnp.dot(zt, filt_ref[0], preferred_element_type=F32)
    one = jnp.dot(zt, filt_ref[1], preferred_element_type=F32)
    two = jnp.dot(zt, filt_ref[2], preferred_element_type=F32)
    outs = []
    for i in range(n):
        one_ref[i, 8:136, :] = one[128 * i : 128 * i + 128]
        two_ref[i, 8:136, :] = two[128 * i : 128 * i + 128]
        one_ref[i, 7:8, :] = carry_ref[0, pl.ds(groups[i], 1), :]
        two_ref[i, 7:8, :] = carry_ref[1, pl.ds(groups[i], 1), :]
        two_ref[i, 6:7, :] = carry_ref[2, pl.ds(groups[i], 1), :]
        total = now[128 * i : 128 * i + 128] + one_ref[i, 7:135, :] + two_ref[i, 6:134, :]
        mix_ref[i, pl.ds(0, 128, stride=2), :] = total[:, :128]
        mix_ref[i, pl.ds(1, 128, stride=2), :] = total[:, 128:]
        outs.append(mix_ref[i].astype(BF))
    return outs


def exchange_kernel(
    x_parts, z_parts, y_parts, c_parts,
    order_hbm, live_ref, volt_ref, table_hbm, beam_hbm, taps_hbm,
    early0, early1, early2, last_ref, filt_out_ref, carry_out_ref,
    order_ref, table_ref, beam_ref, taps_ref, coef_ref, volt, perm, hot, stack, rows, send, recv0, recv1, recv2, filt, ends, edge, tail_send, tail_recv, picked, carry,
    one, two, mix,
    send_sem, recv_sem, edge_sem, out_sem, load_sem, table_sem,
):
    recv = (recv0, recv1, recv2, last_ref)
    early = (early0, early1, early2)
    me = lax.axis_index("sub")
    half = lax.axis_index("tm")
    devices = x_parts * z_parts * y_parts * c_parts
    slots = volt_ref.shape[0]
    live = live_ref[0]
    width = (slots, slots + 1, slots, slots)

    barrier = pltpu.get_barrier_semaphore()

    tail_recv[...] = jnp.zeros_like(tail_recv)
    ends[...] = jnp.zeros_like(ends)

    def greet(i, _):
        @pl.when(i != me)
        def _():
            pl.semaphore_signal(barrier, inc=1, device_id=(i, half), device_id_type=MESH)

        return 0

    lax.fori_loop(0, devices, greet, 0)
    pl.semaphore_signal(barrier, inc=1, device_id=(me, 1 - half), device_id_type=MESH)

    load = [
        pltpu.make_async_copy(volt_ref.at[pl.ds(6 * h, 6)], volt.at[pl.ds(6 * h, 6)], load_sem.at[h])
        for h in range(2)
    ]
    tables = [
        pltpu.make_async_copy(beam_hbm, beam_ref, table_sem.at[0]),
        pltpu.make_async_copy(table_hbm, table_ref, table_sem.at[1]),
        pltpu.make_async_copy(taps_hbm, taps_ref, table_sem.at[2]),
        pltpu.make_async_copy(order_hbm, order_ref, table_sem.at[3]),
    ]
    tables[0].start()
    load[0].start()
    tables[1].start()
    load[1].start()
    for copy in tables[2:]:
        copy.start()
    def fill(i, _):
        ahead = iota((128, 128), 0) + 128 * i - 8 * iota((128, 128), 1)
        for t in range(8):
            perm[pl.ds(pl.multiple_of(128 * i, 128), 128), 128 * t : 128 * t + 128] = (ahead == t).astype(F32).astype(BF)
        return 0

    lax.fori_loop(0, 8, fill, 0)
    tables[0].wait()
    for b in range(4):
        row = iota((128, 256), 0)
        pick = iota((128, 256), 1) == 4 * (row // 2) + b
        key = jnp.sum(
            jnp.where(pick, jnp.broadcast_to(beam_ref[...].astype(F32), (128, 256)), 0.0), axis=1, keepdims=True
        )
        key = key.astype(jnp.int32) + 384 * (iota((128, 1), 0) % 2)
        hot[128 * b : 128 * b + 128, :] = (iota((128, 768), 1) == key).astype(F32).astype(BF)
    for copy in tables[1:]:
        copy.wait()
    stack[...] = jnp.zeros_like(stack)
    part = slots // 2

    def peer(dx, dz, dy, dc):
        c = me % c_parts
        y = (me // c_parts) % y_parts
        z = (me // (c_parts * y_parts)) % z_parts
        x = me // (c_parts * y_parts * z_parts)
        return (
            ((x + dx) % x_parts * z_parts + (z + dz) % z_parts) * y_parts + (y + dy) % y_parts
        ) * c_parts + (c + dc) % c_parts

    def pair(b, j, lo, count):
        dy = j % y_parts
        dz = (j // y_parts) % z_parts
        dc = j // (y_parts * z_parts)
        far = peer(1, dz, dy, dc)
        near = peer(0, dz + z_parts // 2, dy + y_parts // 2, dc)

        def copy(target, i):
            return pltpu.make_async_remote_copy(
                src_ref=send.at[b, target, pl.ds(lo, count)],
                dst_ref=recv[b].at[pl.ds(me * width[b] + lo, count)],
                send_sem=send_sem.at[i, b % 2, j],
                recv_sem=recv_sem.at[b],
                device_id=(target, half),
                device_id_type=MESH,
            )

        return copy(far, 0), copy(near, 1), near != me

    def ship(b, j, first, lo, count):
        far, near, apart = pair(b, j, lo, count)
        if not first:
            old_far, old_near, _ = pair(b - 2, j, 0, width[b - 2])
            old_far.wait_send()
        far.start()

        @pl.when(apart)
        def _():
            if not first:
                old_near.wait_send()
            near.start()

    def ship_range(b, lo, hi, first=False, slot=0, count=None):
        def step(j, _):
            ship(b, j, first, slot, width[b] if count is None else count)
            return 0

        lax.fori_loop(lo, hi, step, 0)

    def sort(s, _):
        parts = [
            jnp.dot(volt[s], perm[:, 256 * n : 256 * n + 256], preferred_element_type=F32).astype(BF)
            for n in range(4)
        ]
        for n in range(4):
            volt[s, :, 256 * n : 256 * n + 256] = parts[n]
        return 0

    def weights(s, lo, hi):
        real, imag = table_ref[s, 0], table_ref[s, 1]
        stack[0:96, 0:320] = real
        stack[0:96, 384:704] = imag
        stack[96:192, 0:320] = -imag
        stack[96:192, 384:704] = real
        return lax.dot_general(hot[lo:hi, :], stack[...], NT, preferred_element_type=F32).astype(BF)

    def form_slot(b, s):
        weight = weights(s, 128 * b, 128 * b + 128)
        for n in range(4):
            out = jnp.dot(weight, volt[s, :, 256 * n : 256 * n + 256], preferred_element_type=F32)
            rows[pl.ds(2 * n, 128, stride=8), :] = out[:, :128]
            rows[pl.ds(2 * n + 1, 128, stride=8), :] = out[:, 128:]
        send[b, :, s] = rows[...].astype(BF).reshape(devices, 16, 128)

    def keep_own(b, lo, hi):
        recv[b][pl.ds(me * width[b] + lo, hi - lo)] = send[b, me, lo:hi]

    def form_beam(b):
        def form(s, _):
            form_slot(b, s)
            return 0

        lax.fori_loop(0, slots, form, 0)
        keep_own(b, 0, width[b])

    def begin(s, _):
        sort(s, 0)
        form_slot(0, s)
        return 0

    hand_on = pltpu.make_async_remote_copy(
        src_ref=tail_send,
        dst_ref=tail_recv,
        send_sem=edge_sem.at[0],
        recv_sem=edge_sem.at[1],
        device_id=(me, 1),
        device_id_type=MESH,
    )

    quarter = part // 2
    for copy in load:
        copy.wait()
    pick_tail = (iota((16, 128), 1) == iota((16, 128), 0) + 112).astype(F32).astype(BF)
    for s in range(slots):
        tail_send[s] = lax.dot_general(pick_tail, volt[s, :, 896:1024], NT, preferred_element_type=F32).astype(BF)
    for lo, count, h in ((0, quarter, 0), (quarter, part - quarter, 0), (part, part, 1)):
        lax.fori_loop(lo, lo + count, begin, 0)
        keep_own(0, lo, lo + count)
        if lo == 0:
            pl.semaphore_wait(barrier, devices)
            @pl.when(half == 0)
            def _():
                hand_on.start()
        ship_range(0, 0, 32, True, lo, count)
    lane = iota((devices, 128), 1)

    def tails(s, _):
        ends[:, 0:16] = lax.dot_general(weights(s, 0, 512), tail_recv[s], NT, preferred_element_type=F32)
        total = jnp.zeros((devices, 128), F32)
        for b in range(4):
            for p in range(2):
                x = ends[pl.ds(128 * b + p, devices, stride=2), :]
                for e in range(2):
                    to = 32 * b + 16 * e + 8 * p
                    moved = pltpu.roll(x, (to - 8 * e) % 128, 1)
                    total = jnp.where((lane >= to) & (lane < to + 8), moved, total)
        edge[pl.ds(s, devices, stride=16), :] = total
        return 0

    @pl.when(half == 0)
    def _():
        hand_on.wait_send()

    @pl.when(half == 1)
    def _():
        hand_on.wait_recv()

    edge[...] = jnp.zeros_like(edge)
    lax.fori_loop(0, slots, tails, 0)
    send[1, :, slots] = edge[...].astype(BF).reshape(devices, 16, 128)
    form_beam(1)
    ship_range(1, 0, 32, True)
    form_beam(2)
    form_beam(3)
    ship_range(2, 0, 32)
    ship_range(3, 0, 32)
    build_filter(taps_ref, coef_ref, filt)
    save_filter = pltpu.make_async_copy(filt, filt_out_ref, out_sem.at[0])
    save_filter.start()

    def arrived(b):
        blocks = (devices - 1) * width[b]
        pltpu.make_async_remote_copy(
            src_ref=recv[b].at[pl.ds(0, blocks)],
            dst_ref=recv[b].at[pl.ds(0, blocks)],
            send_sem=send_sem.at[0, 0],
            recv_sem=recv_sem.at[b],
            device_id=(me, 1 - half),
            device_id_type=MESH,
        ).wait_recv()

    arrived(0)
    arrived(1)
    def unpack(d, _):
        edge[pl.ds(pl.multiple_of(16 * d, 16), 16), :] = recv[1][width[1] * d + slots].astype(F32)
        return 0

    lax.fori_loop(0, devices, unpack, 0)

    def pick(g, _):
        for c in range(16):
            f = 16 * g + c
            slot = order_ref[f]
            row = edge[pl.ds(slot + 4 * (slot // slots), 1), :]
            picked[pl.ds(f, 1), :] = jnp.where(f < live, row, jnp.zeros_like(row))
        return 0

    lax.fori_loop(0, 48, pick, 0)
    lane48 = iota((48, 128), 1)
    for b in range(4):
        sides = []
        for e in range(2):
            halves = []
            for h in range(2):
                acc = jnp.zeros((48, 128), F32)
                for c in range(8):
                    x = picked[pl.ds(8 * h + c, 48, stride=16), :]
                    moved = pltpu.roll(x, (16 * c - (32 * b + 16 * e)) % 128, 1)
                    acc = jnp.where((lane48 >= 16 * c) & (lane48 < 16 * c + 16), moved, acc)
                halves.append(acc.astype(BF))
            sides.append(jnp.concatenate(halves, axis=1))
        before, last = sides
        carry[b, 0] = jnp.dot(last, filt[1], preferred_element_type=F32)
        carry[b, 1] = jnp.dot(last, filt[2], preferred_element_type=F32)
        carry[b, 2] = jnp.dot(before, filt[2], preferred_element_type=F32)
    save_carry = pltpu.make_async_copy(carry.at[3], carry_out_ref, out_sem.at[3])
    save_carry.start()

    for b in range(EARLY):
        if b == 2:
            arrived(2)

        def make(i, _):
            gs = [3 * i + u for u in range(3)]
            bands = [band(recv[b], order_ref, live, g, slots if b == 1 else 0) for g in gs]
            for g, y in zip(gs, synthesise(bands, gs, carry.at[b], filt, one, two, mix)):
                early[b][g] = y
            return 0

        lax.fori_loop(0, 16, make, 0)
    arrived(3)

    def drain(k, _):
        for b in (2, 3):
            far, near, apart = pair(b, k, 0, width[b])
            far.wait_send()

            @pl.when(apart)
            def _():
                near.wait_send()
        return 0

    lax.fori_loop(0, 32, drain, 0)
    save_filter.wait()
    save_carry.wait()


def finish_kernel(
    order_hbm, live_ref, early0, early1, early2, last_ref, filt_ref, carry_ref, out_ref,
    order_ref, filt, carry, stage, one, two, mix, small_sem, out_sem, stage_sem,
):
    small = [
        pltpu.make_async_copy(filt_ref, filt, small_sem.at[0]),
        pltpu.make_async_copy(carry_ref, carry, small_sem.at[1]),
        pltpu.make_async_copy(order_hbm, order_ref, small_sem.at[2]),
    ]
    give = [
        pltpu.make_async_copy(ref, out_ref.at[pl.ds(48 * b, 48)], out_sem.at[b])
        for b, ref in enumerate((early0, early1, early2))
    ]
    for copy in small + give:
        copy.start()

    def put(i):
        return pltpu.make_async_copy(
            stage.at[pl.ds(8 * i, 8)], out_ref.at[pl.ds(48 * EARLY + 8 * i, 8)], stage_sem.at[i]
        )

    for copy in small:
        copy.wait()
    live = live_ref[0]

    def make(i, _):
        gs = [8 * i + u for u in range(8)]
        bands = [band(last_ref, order_ref, live, g) for g in gs]
        for g, y in zip(gs, synthesise(bands, gs, carry, filt, one, two, mix)):
            stage[g] = y
        put(i).start()
        return 0

    lax.fori_loop(0, 6, make, 0)

    def close(i, _):
        put(i).wait()
        return 0

    lax.fori_loop(0, 6, close, 0)
    for copy in give:
        copy.wait()


def on_device(sizes, voltages, pointing_table, beam_pointing, subband_order, live_subbands, filter_taps):
    slots = voltages.shape[0]
    devices = sizes[0] * sizes[1] * sizes[2] * sizes[3]
    volt = voltages.reshape(slots, 192, 1024)
    table = jnp.swapaxes(pointing_table, 2, 3)
    beams = beam_pointing.reshape(1, 256)
    table, beams, filter_taps, subband_order = (
        pltpu.with_memory_space_constraint(a, pltpu.HBM) for a in (table, beams, filter_taps, subband_order)
    )
    smem = pl.BlockSpec(memory_space=pltpu.SMEM)
    vmem = pl.BlockSpec(memory_space=pltpu.VMEM)
    hbm = pl.BlockSpec(memory_space=pltpu.HBM)
    VM = pltpu.VMEM
    def synth_scratch(n):
        return [VM((n, 136, 256), F32), VM((n, 136, 256), F32), VM((n, 256, 128), F32)]

    early0, early1, early2, last, filt, carry = pl.pallas_call(
        functools.partial(exchange_kernel, *sizes),
        name="exchange",
        out_shape=[
            *[jax.ShapeDtypeStruct((48, 256, 128), BF)] * EARLY,
            jax.ShapeDtypeStruct((devices * slots, 16, 128), BF),
            jax.ShapeDtypeStruct((3, 256, 256), BF),
            jax.ShapeDtypeStruct((3, 48, 256), F32),
        ],
        in_specs=[hbm, smem, hbm, hbm, hbm, hbm],
        out_specs=[vmem] * 4 + [hbm] * 2,
        scratch_shapes=[
            pltpu.SMEM((768,), jnp.int32),
            VM((slots, 2, 96, 320), BF),
            VM((1, 256), jnp.int32),
            VM((16, 16), F32),
            VM((64, 128), F32),
            VM((slots, 192, 1024), BF),
            VM((1024, 1024), BF),
            VM((512, 768), BF),
            VM((192, 768), BF),
            VM((1024, 128), F32),
            VM((4, devices, slots + 1, 16, 128), BF),
            VM((devices * slots, 16, 128), BF),
            VM((devices * (slots + 1), 16, 128), BF),
            VM((devices * slots, 16, 128), BF),
            VM((3, 256, 256), BF),
            VM((512, 128), F32),
            VM((16 * devices, 128), F32),
            VM((slots, 16, 192), BF),
            VM((slots, 16, 192), BF),
            VM((768, 128), F32),
            VM((4, 3, 48, 256), F32),
            *synth_scratch(3),
            pltpu.SemaphoreType.DMA((2, 2, 32)),
            pltpu.SemaphoreType.DMA((4,)),
            pltpu.SemaphoreType.DMA((2,)),
            pltpu.SemaphoreType.DMA((4,)),
            pltpu.SemaphoreType.DMA((2,)),
            pltpu.SemaphoreType.DMA((4,)),
        ],
        compiler_params=pltpu.CompilerParams(
            collective_id=0, has_side_effects=True, vmem_limit_bytes=39 * 1024 * 1024
        ),
    )(subband_order, live_subbands, volt, table, beams, filter_taps)

    out = pl.pallas_call(
        finish_kernel,
        name="finish",
        out_shape=jax.ShapeDtypeStruct((192, 256, 128), BF),
        in_specs=[hbm, smem, vmem, vmem, vmem, vmem, hbm, hbm],
        out_specs=hbm,
        scratch_shapes=[
            pltpu.SMEM((768,), jnp.int32),
            VM((3, 256, 256), BF),
            VM((3, 48, 256), F32),
            VM((48, 256, 128), BF),
            *synth_scratch(8),
            pltpu.SemaphoreType.DMA((3,)),
            pltpu.SemaphoreType.DMA((3,)),
            pltpu.SemaphoreType.DMA((6,)),
        ],
        compiler_params=pltpu.CompilerParams(vmem_limit_bytes=12 * 1024 * 1024),
    )(subband_order, live_subbands, early0, early1, early2, last, filt, carry)
    out = out.reshape(4, 48, 128, 2, 128)
    return jnp.swapaxes(out, 2, 3).reshape(4, 48, 2, 16384)


def solution(mesh):
    sizes = (2, 4, 4, 2)
    in_specs = (P("sub", None, None, "tm"), P("sub", None, None, None), P(), P(), P(), P())
    out_specs = P("sub", None, None, "tm")
    return jax.shard_map(
        functools.partial(on_device, sizes), mesh=mesh, in_specs=in_specs, out_specs=out_specs, check_vma=False
    )
```
